16 devices in a mesh: dp: 2 (over z), ep: 8 (over y, x, core).
Axes of the slice: x: 2, y: 2, z: 2, core: 2. Of those that a mesh axis runs over, the one named last changes fastest.
Arguments:
- x_norm: bfloat16 [8192, 4096], P(('dp', 'ep'))
- route_idx: int32 [8192, 2], P(('dp', 'ep'))
- w_router: bfloat16 [4096, 16], replicated
- w_gate: bfloat16 [16, 4096, 688], P('ep')
- w_up: bfloat16 [16, 4096, 688], P('ep')
- w_down: bfloat16 [16, 688, 4096], P('ep')
- grad_out: bfloat16 [8192, 4096], P(('dp', 'ep'))
Outputs:
- output 1: bfloat16 [8192, 4096], P(('dp', 'ep'))
- output 2: float32 [16, 4096, 688], P('ep')
- output 3: float32 [16, 4096, 688], P('ep')
- output 4: float32 [16, 688, 4096], P('ep')
- output 5: float32 [4096, 16], replicated
All inputs are finite; a program needn't handle non-finite values.
Results may differ from the reference program's by a relative error of at most 0.0058515.
Values are sent between devices in bfloat16 or wider.
A program may use at most 1 GiB of HBM per device.

```python
import jax
import jax.numpy as jnp
from jax import lax

D = 4096
FF = 688
EXPERTS = 16
TOP = 2
TOK_DEV = 512
SHARDS = 16
CAP = 192
TOKENS = SHARDS * TOK_DEV
N_CHOICE = TOKENS * TOP


def shuffle_rows(row_key):
    return jax.random.permutation(row_key, TOK_DEV)


def permute_rows(shard_rows, row_order):
    return shard_rows[row_order]


def draw_routes(route_key):
    perm_key, shift_key, order_key = jax.random.split(route_key, 3)
    expert_order = jax.random.permutation(perm_key, EXPERTS).astype(jnp.int32)
    shifts = jax.random.randint(shift_key, (SHARDS,), 0, EXPERTS - 1, dtype=jnp.int32)
    tok_pos = jnp.arange(TOK_DEV, dtype=jnp.int32)
    choice_pos = jnp.arange(TOP, dtype=jnp.int32)
    is_hot = tok_pos < CAP
    cycle_pos = (tok_pos * TOP - jnp.minimum(tok_pos, CAP))[:, None] + choice_pos[None, :] - is_hot[:, None].astype(jnp.int32)
    labels = 1 + (cycle_pos[None, :, :] + shifts[:, None, None]) % (EXPERTS - 1)
    hot_slot = is_hot[:, None] & (choice_pos[None, :] == 0)
    labels = jnp.where(hot_slot[None, :, :], 0, labels)
    experts = expert_order[labels]
    row_orders = jax.vmap(shuffle_rows)(jax.random.split(order_key, SHARDS))
    experts = jax.vmap(permute_rows)(experts, row_orders)
    return experts.reshape(TOKENS, TOP).astype(jnp.int32)


def setup_inputs(seed: int = 0) -> dict:
    base_key = jax.random.key(seed)
    key_list = jax.random.split(base_key, 7)
    x_norm = jax.random.normal(key_list[0], (TOKENS, D), jnp.float32)
    w_router = jax.random.normal(key_list[2], (D, EXPERTS), jnp.float32) * D ** -0.5
    w_gate = jax.random.normal(key_list[3], (EXPERTS, D, FF), jnp.float32) * D ** -0.5
    w_up = jax.random.normal(key_list[4], (EXPERTS, D, FF), jnp.float32) * D ** -0.5
    w_down = jax.random.normal(key_list[5], (EXPERTS, FF, D), jnp.float32) * FF ** -0.5
    grad_out = jax.random.normal(key_list[6], (TOKENS, D), jnp.float32)
    return {
        "x_norm": x_norm.astype(jnp.bfloat16),
        "route_idx": draw_routes(key_list[1]),
        "w_router": w_router.astype(jnp.bfloat16),
        "w_gate": w_gate.astype(jnp.bfloat16),
        "w_up": w_up.astype(jnp.bfloat16),
        "w_down": w_down.astype(jnp.bfloat16),
        "grad_out": grad_out.astype(jnp.bfloat16),
    }


def expert_backward(x_rows, dy_rows, gate_rows, w_gate_e, w_up_e, w_down_e):
    z_gate = jnp.dot(x_rows, w_gate_e, preferred_element_type=jnp.float32)
    z_up = jnp.dot(x_rows, w_up_e, preferred_element_type=jnp.float32)
    sigmoid_z = jax.nn.sigmoid(z_gate)
    silu_z = z_gate * sigmoid_z
    act_rows = (silu_z * z_up).astype(jnp.bfloat16)
    out_rows = jnp.dot(act_rows, w_down_e, preferred_element_type=jnp.float32)
    dy_wide = dy_rows.astype(jnp.float32)
    dgate_rows = jnp.sum(out_rows * dy_wide, axis=1)
    d_out = (gate_rows[:, None] * dy_wide).astype(jnp.bfloat16)
    d_act = jnp.dot(d_out, w_down_e.T, preferred_element_type=jnp.float32)
    d_zgate = (d_act * z_up * sigmoid_z * (1.0 + z_gate * (1.0 - sigmoid_z))).astype(jnp.bfloat16)
    d_zup = (d_act * silu_z).astype(jnp.bfloat16)
    dx_rows = (jnp.dot(d_zgate, w_gate_e.T, preferred_element_type=jnp.float32) + jnp.dot(d_zup, w_up_e.T, preferred_element_type=jnp.float32)).astype(jnp.bfloat16)
    grad_gate = jnp.dot(x_rows.T, d_zgate, preferred_element_type=jnp.float32)
    grad_up = jnp.dot(x_rows.T, d_zup, preferred_element_type=jnp.float32)
    grad_down = jnp.dot(act_rows.T, d_out, preferred_element_type=jnp.float32)
    return dx_rows, dgate_rows, grad_gate, grad_up, grad_down


def reference(x_norm, route_idx, w_router, w_gate, w_up, w_down, grad_out):
    logits = jnp.dot(x_norm, w_router, preferred_element_type=jnp.float32)
    gate_probs = jax.nn.softmax(jnp.take_along_axis(logits, route_idx, axis=1), axis=-1)
    expert_ids = jnp.arange(EXPERTS, dtype=jnp.int32)
    shard_idx = route_idx.reshape(SHARDS, TOK_DEV * TOP)
    one_hot = (shard_idx[:, :, None] == expert_ids).astype(jnp.int32)
    rank_in = jnp.sum((jnp.cumsum(one_hot, axis=1) - one_hot) * one_hot, axis=2)
    slot_ids = (shard_idx * (SHARDS * CAP) + jnp.arange(SHARDS, dtype=jnp.int32)[:, None] * CAP + rank_in).reshape(N_CHOICE)
    slot_table = jnp.full((EXPERTS * SHARDS * CAP,), N_CHOICE, jnp.int32).at[slot_ids].set(jnp.arange(N_CHOICE, dtype=jnp.int32)).reshape(EXPERTS, SHARDS * CAP)
    gate_flat = gate_probs.reshape(N_CHOICE)

    def one_expert(operands):
        w_gate_e, w_up_e, w_down_e, choice_ids = operands
        is_valid = choice_ids < N_CHOICE
        safe_ids = jnp.minimum(choice_ids, N_CHOICE - 1)
        x_rows = jnp.where(is_valid[:, None], x_norm[safe_ids // TOP], 0.0)
        dy_rows = jnp.where(is_valid[:, None], grad_out[safe_ids // TOP], 0.0)
        gate_rows = jnp.where(is_valid, gate_flat[safe_ids], 0.0)
        return expert_backward(x_rows, dy_rows, gate_rows, w_gate_e, w_up_e, w_down_e)

    dx_rows, dgate_rows, grad_gate, grad_up, grad_down = lax.map(one_expert, (w_gate, w_up, w_down, slot_table))
    dx_choice = dx_rows.reshape(EXPERTS * SHARDS * CAP, D)[slot_ids].reshape(TOKENS, TOP, D)
    dgate = dgate_rows.reshape(EXPERTS * SHARDS * CAP)[slot_ids].reshape(TOKENS, TOP)
    d_sel = gate_probs * (dgate - jnp.sum(gate_probs * dgate, axis=1, keepdims=True))
    d_logits = jnp.sum(jnp.where(route_idx[:, :, None] == expert_ids, d_sel[:, :, None], 0.0), axis=1).astype(jnp.bfloat16)
    du_router = jnp.dot(d_logits, w_router.T, preferred_element_type=jnp.float32)
    grad_x = (jnp.sum(dx_choice.astype(jnp.float32), axis=1) + du_router).astype(jnp.bfloat16)
    grad_router = jnp.dot(x_norm.T, d_logits, preferred_element_type=jnp.float32)
    return grad_x, grad_gate, grad_up, grad_down, grad_router
```

```python
import jax
import jax.numpy as jnp
from jax import lax
from jax.experimental import pallas as pl
from jax.experimental.pallas import tpu as pltpu
from jax.sharding import PartitionSpec as P

TILE = 512
GRP = 16
SLOT = 256
NT_DIMS = (((1,), (1,)), ((), ()))
TN_DIMS = (((0,), (0,)), ((), ()))
VMEM = 63 * 2**20
BF = jnp.bfloat16
F32 = jnp.float32


def params(**kw):
    return pltpu.CompilerParams(vmem_limit_bytes=VMEM, **kw)


def cost(flops, nbytes):
    return pl.CostEstimate(flops=int(flops), bytes_accessed=int(nbytes), transcendentals=0)


def pick_rows(slot0, slot1, n_tok):
    row = lax.broadcasted_iota(jnp.int32, (SLOT, n_tok), 0)
    return row == slot0, row == slot1


def gather_rows(order, dst, slot0, slot1, p0, p1, rows_all, n_rows, with_p):
    n_steps = order.shape[0]
    n_tok = slot0.shape[-1]
    dim = rows_all.shape[1]
    per = SLOT // GRP
    chunk = 1024

    def body(order_ref, dst_ref, s0_ref, s1_ref, p0_ref, p1_ref, x_ref, *rest):
        if with_p:
            o_ref, po_ref, buf, pbuf, sems, psems = rest
        else:
            o_ref, buf, sems = rest
        i = pl.program_id(0)
        now = lax.rem(i, 2)

        def copies(step, half, j):
            d = dst_ref[step * per + j]
            at = pl.multiple_of(jnp.maximum(d, 0) * GRP, GRP)
            out = [pltpu.make_async_copy(buf.at[half, pl.ds(j * GRP, GRP)], o_ref.at[pl.ds(at, GRP)], sems.at[half, j])]
            if with_p:
                out.append(pltpu.make_async_copy(pbuf.at[half, pl.ds(j * GRP, GRP)], po_ref.at[pl.ds(at, GRP)], psems.at[half, j]))
            return d, out

        def each(step, half, wait):
            for j in range(per):
                d, cs = copies(step, half, j)

                @pl.when(d >= 0)
                def _():
                    for c in cs:
                        if wait:
                            c.wait()
                        else:
                            c.start()

        @pl.when(i >= 2)
        def _():
            each(i - 2, now, True)

        is0, is1 = pick_rows(s0_ref[0], s1_ref[0], n_tok)
        pick = jnp.where(is0 | is1, 1.0, 0.0).astype(BF)
        for c in range(dim // chunk):
            cols = pl.ds(c * chunk, chunk)
            buf[now, :, cols] = jnp.dot(pick, x_ref[:, cols], preferred_element_type=F32).astype(BF)
        if with_p:
            p = jnp.where(is0, p0_ref[0], 0.0) + jnp.where(is1, p1_ref[0], 0.0)
            pbuf[now] = jnp.broadcast_to(jnp.sum(p, axis=1, keepdims=True), (SLOT, 128))
        each(i, now, False)

        @pl.when(i == n_steps - 1)
        def _():
            each(i - 1, 1 - now, True)
            each(i, now, True)

    vec = pl.BlockSpec((1, 1, n_tok), lambda i, o, d: (i, 0, 0))
    outs = [jax.ShapeDtypeStruct((n_rows, dim), BF)]
    scratch = [pltpu.VMEM((2, SLOT, dim), BF), pltpu.SemaphoreType.DMA((2, per))]
    if with_p:
        outs.append(jax.ShapeDtypeStruct((n_rows, 128), F32))
        scratch = [scratch[0], pltpu.VMEM((2, SLOT, 128), F32), scratch[1], pltpu.SemaphoreType.DMA((2, per))]
    return pl.pallas_call(
        body,
        grid_spec=pltpu.PrefetchScalarGridSpec(
            num_scalar_prefetch=2,
            grid=(n_steps,),
            in_specs=[vec, vec, vec, vec, pl.BlockSpec((n_tok, dim), lambda i, o, d: (o[i], 0))],
            out_specs=[pl.BlockSpec(memory_space=pl.ANY)] * len(outs),
            scratch_shapes=scratch,
        ),
        out_shape=outs,
        compiler_params=params(),
        cost_estimate=cost(2 * n_steps * SLOT * n_tok * dim, rows_all.size * 2 + n_rows * dim * 2),
        name="gather_p" if with_p else "gather_g",
    )(order, dst, slot0, slot1, p0, p1, rows_all)


def forward(tile_e, n_tiles, xs, w1, w3):
    n_rows, dim = xs.shape
    ff = w1.shape[1]
    nt = n_rows // TILE

    def body(te, ntr, x_ref, w1_ref, w3_ref, a_ref, u1_ref, u3_ref):
        @pl.when(pl.program_id(0) < ntr[0])
        def _():
            z1 = lax.dot_general(x_ref[...], w1_ref[0], NT_DIMS, preferred_element_type=F32)
            z3 = lax.dot_general(x_ref[...], w3_ref[0], NT_DIMS, preferred_element_type=F32)
            sg = jax.nn.sigmoid(z1)
            s = z1 * sg
            a_ref[...] = (s * z3).astype(BF)
            u1_ref[...] = z3 * sg * (1.0 + z1 * (1.0 - sg))
            u3_ref[...] = s

    at = lambda t, te, n: (jnp.minimum(t, n[0] - 1), 0)
    wt = pl.BlockSpec((1, ff, dim), lambda t, te, n: (te[t], 0, 0))
    rf = pl.BlockSpec((TILE, ff), at)
    return pl.pallas_call(
        body,
        grid_spec=pltpu.PrefetchScalarGridSpec(
            num_scalar_prefetch=2,
            grid=(nt,),
            in_specs=[pl.BlockSpec((TILE, dim), at), wt, wt],
            out_specs=[rf, rf, rf],
        ),
        out_shape=[jax.ShapeDtypeStruct((n_rows, ff), d) for d in (BF, F32, F32)],
        compiler_params=params(),
        cost_estimate=cost(4 * n_rows * dim * ff, n_rows * dim * 2),
        name="forward",
    )(tile_e, n_tiles, xs, w1, w3)


def hidden_grad(tile_e, n_tiles, gs, ps, a, u1, u3, w2):
    n_rows, dim = gs.shape
    ff = w2.shape[1]
    nt = n_rows // TILE

    def body(te, ntr, g_ref, p_ref, a_ref, u1_ref, u3_ref, w_ref, d1_ref, d3_ref, q_ref):
        @pl.when(pl.program_id(0) < ntr[0])
        def _():
            h = lax.dot_general(g_ref[...], w_ref[0], NT_DIMS, preferred_element_type=F32)
            q = jnp.sum(a_ref[...].astype(F32) * h, axis=1, keepdims=True)
            q_ref[...] = jnp.broadcast_to(q, q_ref.shape)
            da = p_ref[:, 0:1] * h
            d1_ref[...] = (da * u1_ref[...]).astype(BF)
            d3_ref[...] = (da * u3_ref[...]).astype(BF)

    at = lambda t, te, n: (jnp.minimum(t, n[0] - 1), 0)
    rf = pl.BlockSpec((TILE, ff), at)
    lane = pl.BlockSpec((TILE, 128), at)
    return pl.pallas_call(
        body,
        grid_spec=pltpu.PrefetchScalarGridSpec(
            num_scalar_prefetch=2,
            grid=(nt,),
            in_specs=[pl.BlockSpec((TILE, dim), at), lane, rf, rf, rf, pl.BlockSpec((1, ff, dim), lambda t, te, n: (te[t], 0, 0))],
            out_specs=[rf, rf, lane],
        ),
        out_shape=[jax.ShapeDtypeStruct((n_rows, ff), BF)] * 2 + [jax.ShapeDtypeStruct((n_rows, 128), F32)],
        compiler_params=params(),
        cost_estimate=cost(2 * n_rows * dim * ff, n_rows * dim * 2),
        name="hidden_grad",
    )(tile_e, n_tiles, gs, ps, a, u1, u3, w2)


def row_grad(tiles, tiles_e, n_tiles, inverse, d1, d3, w1, w3, n_out, first, width):
    ff = d1.shape[1]
    nl = tiles.shape[0]
    per = TILE // GRP
    chunk = min(width, 1024)

    def body(tl, te, ntr, inv, d1_ref, d3_ref, w1_ref, w3_ref, o_ref, buf, sems):
        t = pl.program_id(0)
        now = lax.rem(t, 2)

        def each(step, half, wait):
            for j in range(per):
                d = inv[tl[step] * per + j]
                at = pl.multiple_of(jnp.maximum(d, 0) * GRP, GRP)

                @pl.when((step < ntr[0]) & (d >= 0))
                def _():
                    c = pltpu.make_async_copy(buf.at[half, pl.ds(j * GRP, GRP)], o_ref.at[pl.ds(at, GRP)], sems.at[half, j])
                    if wait:
                        c.wait()
                    else:
                        c.start()

        @pl.when(t >= 2)
        def _():
            each(t - 2, now, True)

        @pl.when(t < ntr[0])
        def _():
            for c in range(width // chunk):
                cols = pl.ds(c * chunk, chunk)
                r = jnp.dot(d1_ref[...], w1_ref[0, :, cols], preferred_element_type=F32)
                r += jnp.dot(d3_ref[...], w3_ref[0, :, cols], preferred_element_type=F32)
                buf[now, :, cols] = r.astype(BF)

        each(t, now, False)

        @pl.when(t == nl - 1)
        def _():
            each(t - 1, 1 - now, True)
            each(t, now, True)

    at = pl.BlockSpec((TILE, ff), lambda t, tl, te, n, inv: (tl[t], 0))
    wt = pl.BlockSpec((1, ff, width), lambda t, tl, te, n, inv: (te[t], 0, first // width))
    return pl.pallas_call(
        body,
        grid_spec=pltpu.PrefetchScalarGridSpec(
            num_scalar_prefetch=4,
            grid=(nl,),
            in_specs=[at, at, wt, wt],
            out_specs=pl.BlockSpec(memory_space=pl.ANY),
            scratch_shapes=[pltpu.VMEM((2, TILE, width), BF), pltpu.SemaphoreType.DMA((2, per))],
        ),
        out_shape=jax.ShapeDtypeStruct((n_out, width), BF),
        compiler_params=params(),
        cost_estimate=cost(4 * nl * TILE * width * ff, n_out * width * 2),
        name="row_grad",
    )(tiles, tiles_e, n_tiles, inverse, d1, d3, w1, w3)


def weight_grads(tile_e, n_tiles, xs, gs, ps, a, d1, d3):
    n_rows, dim = xs.shape
    ff = a.shape[1]
    nt = n_rows // TILE
    cols = 1024

    def body(te, ntr, x_ref, g_ref, p_ref, a_ref, d1_ref, d3_ref, o1_ref, o3_ref, o2_ref):
        t = pl.program_id(1)
        fresh = (t == 0) | (te[t] != te[jnp.maximum(t - 1, 0)])

        @pl.when(t < ntr[0])
        def _():
            x = x_ref[...]
            do = (p_ref[:, 0:1] * g_ref[...].astype(F32)).astype(BF)
            for lhs, rhs, out in ((d1_ref, x, o1_ref), (d3_ref, x, o3_ref), (a_ref, do, o2_ref)):
                new = lax.dot_general(lhs[...], rhs, TN_DIMS, preferred_element_type=F32)

                @pl.when(fresh)
                def _():
                    out[0] = new

                @pl.when(jnp.logical_not(fresh))
                def _():
                    out[0] += new

    tc = lambda t, n: jnp.minimum(t, n[0] - 1)
    wide = pl.BlockSpec((TILE, cols), lambda d, t, te, n: (tc(t, n), d))
    rf = pl.BlockSpec((TILE, ff), lambda d, t, te, n: (tc(t, n), 0))
    lane = pl.BlockSpec((TILE, 128), lambda d, t, te, n: (tc(t, n), 0))
    out = pl.BlockSpec((1, ff, cols), lambda d, t, te, n: (te[t], 0, d))
    return pl.pallas_call(
        body,
        grid_spec=pltpu.PrefetchScalarGridSpec(
            num_scalar_prefetch=2,
            grid=(dim // cols, nt),
            in_specs=[wide, wide, lane, rf, rf, rf],
            out_specs=[out, out, out],
        ),
        out_shape=[jax.ShapeDtypeStruct((2, ff, dim), F32)] * 3,
        compiler_params=params(),
        cost_estimate=cost(6 * n_rows * dim * ff, 4 * n_rows * dim + 12 * ff * dim * 2),
        name="weight_grads",
    )(tile_e, n_tiles, xs, gs, ps, a, d1, d3)


def combine(valid, i0, i1, dl, wr_t, blocks):
    n_tok = i0.shape[0]
    dim = wr_t.shape[1]
    n_src = len(blocks[0])
    width = blocks[0][0].shape[1]
    cols = 512
    per = width // cols
    n_half = len(blocks)

    def body(nv, i0_ref, i1_ref, dl_ref, w_ref, *rest):
        refs, o_ref, pick = rest[: n_src * n_half], rest[-2], rest[-1]
        c = pl.program_id(0)

        @pl.when(c == 0)
        def _():
            col = lax.broadcasted_iota(jnp.int32, (n_tok, n_src * SLOT), 1)
            pick[...] = jnp.where((col == i0_ref[...]) | (col == i1_ref[...]), 1.0, 0.0).astype(BF)

        for h in range(n_half):

            @pl.when((c >= h * per) & (c < (h + 1) * per))
            def _():
                acc = jnp.dot(dl_ref[...], w_ref[...], preferred_element_type=F32)
                row = lax.broadcasted_iota(jnp.int32, (SLOT, cols), 0)
                tot = jnp.zeros((n_tok, cols), F32)
                for b in range(n_src):
                    blk = jnp.where(row < nv[b], refs[h * n_src + b][...].astype(F32), 0.0).astype(BF)
                    tot += jnp.dot(pick[:, b * SLOT : (b + 1) * SLOT], blk, preferred_element_type=F32)
                o_ref[...] = (tot + acc).astype(BF)

    one = pl.BlockSpec((n_tok, 1), lambda c, nv: (0, 0))
    ins = [one, one, pl.BlockSpec((n_tok, dl.shape[1]), lambda c, nv: (0, 0)), pl.BlockSpec((dl.shape[1], cols), lambda c, nv: (0, c))]
    for h in range(n_half):
        ins += [pl.BlockSpec((SLOT, cols), lambda c, nv, h=h: (0, jnp.clip(c - h * per, 0, per - 1)))] * n_src
    return pl.pallas_call(
        body,
        grid_spec=pltpu.PrefetchScalarGridSpec(
            num_scalar_prefetch=1,
            grid=(dim // cols,),
            in_specs=ins,
            out_specs=pl.BlockSpec((n_tok, cols), lambda c, nv: (0, c)),
            scratch_shapes=[pltpu.VMEM((n_tok, n_src * SLOT), BF)],
        ),
        out_shape=jax.ShapeDtypeStruct((n_tok, dim), BF),
        compiler_params=params(),
        cost_estimate=cost(2 * n_tok * n_src * SLOT * dim, n_src * SLOT * dim * 2),
        name="combine",
    )(valid, i0, i1, dl, wr_t, *[b for half in blocks for b in half])


def up(v, m):
    return (v + m - 1) // m * m


def before(v):
    n = v.shape[0]
    i = jnp.arange(n, dtype=jnp.int32)
    return jnp.sum(jnp.where(i[None, :] < i[:, None], v[None, :], 0), axis=1)


def running(mask):
    n = mask.shape[-1]
    i = jnp.arange(n, dtype=jnp.int32)
    tri = (i[:, None] <= i[None, :]).astype(BF)
    return jnp.dot(mask.astype(BF), tri, preferred_element_type=F32).astype(jnp.int32)


def solution(mesh):
    n_dp, n_ep = mesh.shape["dp"], mesh.shape["ep"]
    tok_spec = P(("dp", "ep"), None)
    exp_spec = P("ep", None, None)
    both = ("dp", "ep")

    def device_step(x_loc, route_idx, w_router, w_gate, w_up, w_down, g_loc):
        n_tok, top_k = route_idx.shape
        dim = x_loc.shape[1]
        n_exp = w_router.shape[1]
        my_dp, my_ep = lax.axis_index("dp"), lax.axis_index("ep")
        n_sh = n_dp * n_ep
        per = SLOT // GRP
        fill = TILE // GRP
        n_rows = (n_sh * SLOT // TILE + 1) * TILE
        nt = n_rows // TILE
        i32 = jnp.int32

        x_all = lax.all_gather(x_loc, both, axis=0, tiled=True)
        g_all = lax.all_gather(g_loc, both, axis=0, tiled=True)

        w1 = jnp.swapaxes(w_gate, 1, 2)
        w3 = jnp.swapaxes(w_up, 1, 2)
        wr_t = w_router.T

        logits = lax.dot_general(wr_t, x_loc, NT_DIMS, preferred_element_type=F32)
        idx = route_idx.T
        eid = jnp.arange(n_exp, dtype=i32)
        hot = [idx[k][None, :] == eid[:, None] for k in range(top_k)]
        sel = jnp.stack([jnp.sum(jnp.where(h, logits, 0.0), axis=0) for h in hot])
        probs = jax.nn.softmax(sel, axis=0)
        meta = lax.all_gather(jnp.concatenate([idx.astype(F32), probs]), both, axis=0)

        step = jnp.arange(n_sh, dtype=i32)
        order = ((my_dp + step // n_ep) % n_dp) * n_ep + ((step % n_ep) ^ my_ep)
        meta = meta[order]
        i_all, p_all = meta[:, :top_k].astype(i32), meta[:, top_k:]
        e0 = my_ep * 2
        m0 = [i_all[:, k] == e0 for k in range(top_k)]
        m1 = [i_all[:, k] == e0 + 1 for k in range(top_k)]
        m0, m1, p0, p1 = m0[0] | m0[1], m1[0] | m1[1], jnp.where(m0[0], p_all[:, 0], p_all[:, 1]), jnp.where(m1[0], p_all[:, 0], p_all[:, 1])
        run = running(jnp.concatenate([m0, m1]))
        r0, r1 = run[:n_sh], run[n_sh:]
        k0, k1 = up(r0[:, -1], GRP) // GRP, up(r1[:, -1], GRP) // GRP
        slot0 = jnp.where(m0, r0 - 1, -1)
        slot1 = jnp.where(m1, k0[:, None] * GRP + r1 - 1, -1)
        t0, t1 = jnp.sum(k0), jnp.sum(k1)
        n0, n1 = up(t0, fill) // fill, up(t1, fill) // fill
        n_tiles = n0 + n1
        s0, s1 = before(k0), n0 * fill + before(k1)
        j = jnp.arange(per, dtype=i32)[None, :]
        dst = jnp.where(j < k0[:, None], s0[:, None] + j, jnp.where(j < (k0 + k1)[:, None], s1[:, None] + j - k0[:, None], -1))
        f = jnp.arange(fill, dtype=i32)
        gap0 = jnp.where(t0 + f < n0 * fill, t0 + f, -1)
        gap1 = jnp.where(t1 + f < n1 * fill, n0 * fill + t1 + f, -1)
        dst_all = jnp.concatenate([dst.reshape(-1), gap0, gap1])
        n_fill = 2 * fill // per
        order_all = jnp.concatenate([order, jnp.broadcast_to(order[-1], (n_fill,))])
        pad = lambda v, c: jnp.concatenate([v, jnp.full((n_fill, n_tok), c, v.dtype)])[:, None, :]
        slot0, slot1, p0, p1 = pad(slot0, -1), pad(slot1, -1), pad(p0, 0.0), pad(p1, 0.0)
        tiles = jnp.arange(nt, dtype=i32)
        tile_e = (tiles >= n0).astype(i32)
        count = n_tiles[None]

        dst_loc = dst[:n_ep]
        back = dst_loc.reshape(-1)
        grp = jnp.arange(nt * fill, dtype=i32)
        inverse = jnp.sum(jnp.where(back[:, None] == grp[None, :], jnp.arange(n_ep * per, dtype=i32)[:, None] + 1, 0), axis=0) - 1
        l0, l1 = up(jnp.sum(k0[:n_ep]), fill) // fill, up(jnp.sum(k1[:n_ep]), fill) // fill
        nl = n_ep * SLOT // TILE + 1
        lt = jnp.arange(nl, dtype=i32)
        loc_e = (lt >= l0).astype(i32)
        loc_t = jnp.where(lt < l0, lt, n0 + jnp.minimum(lt, l0 + l1 - 1) - l0)
        loc_n = (l0 + l1)[None]

        mine = jnp.concatenate(hot)
        rank = running(mine)
        cnt = rank[:n_exp] + rank[n_exp:]
        kk = up(cnt[:, -1], GRP)
        off = jnp.where(eid % 2 == 1, jnp.concatenate([kk[:1], kk[:-1]]), 0)
        slot = off[:, None] + cnt - 1
        own = [jnp.sum(jnp.where(h, slot, 0), axis=0) for h in hot]
        src = [idx[k] // 2 for k in range(top_k)]
        nat = [src[k] * SLOT + own[k] for k in range(top_k)]
        ret = [((src[k] ^ my_ep) * SLOT + own[k])[:, None] for k in range(top_k)]
        dev = jnp.arange(n_ep, dtype=i32)
        full = kk.reshape(n_ep, 2).sum(axis=1)
        valid = jnp.sum(jnp.where((dev ^ my_ep)[:, None] == dev[None, :], full[None, :], 0), axis=1)

        xs, ps = gather_rows(order_all, dst_all, slot0, slot1, p0, p1, x_all, n_rows, True)
        a, u1, u3 = forward(tile_e, count, xs, w1, w3)

        (gs,) = gather_rows(order_all, dst_all, slot0, slot1, p0, p1, g_all, n_rows, False)
        d1, d3, q = hidden_grad(tile_e, count, gs, ps, a, u1, u3, w_down)

        nat_dst = dst_loc[dev ^ my_ep].reshape(-1)
        q_send = q[:, 0].reshape(nt * fill, GRP)[jnp.maximum(nat_dst, 0)].reshape(n_ep, SLOT)
        q_recv = lax.all_to_all(q_send, "ep", 0, 0, tiled=True).reshape(1, n_ep * SLOT)
        spot = jnp.arange(n_ep * SLOT, dtype=i32)[None, :]
        qk = [jnp.sum(jnp.where(spot == nat[k][:, None], q_recv, 0.0), axis=1) for k in range(top_k)]
        mean = probs[0] * qk[0] + probs[1] * qk[1]
        dl = [probs[k] * (qk[k] - mean) for k in range(top_k)]
        d_logits = sum(jnp.where(idx[k][:, None] == eid[None, :], dl[k][:, None], 0.0) for k in range(top_k)).astype(BF)
        part_router = lax.dot_general(d_logits, x_loc, TN_DIMS, preferred_element_type=F32)
        grad_router = lax.psum(part_router, both).T

        n_half = 2
        width = dim // n_half
        rows = [row_grad(loc_t, loc_e, loc_n, inverse, d1, d3, w1, w3, n_ep * SLOT, h * width, width) for h in range(n_half)]
        blocks = []
        for h in range(n_half):
            got = [rows[h][:SLOT]]
            for b in range(1, n_ep):
                part = rows[h][b * SLOT : (b + 1) * SLOT]
                got.append(lax.ppermute(part, "ep", [(s, s ^ b) for s in range(n_ep)]))
            blocks.append(got)

        d1b, d3b, _, _ = lax.optimization_barrier((d1, d3, rows[-1][:8, :128], part_router))
        o1, o3, o2 = weight_grads(tile_e, count, xs, gs, ps, a, d1b, d3b)
        grad_x = combine(valid, ret[0], ret[1], d_logits, wr_t, blocks)
        return grad_x, jnp.swapaxes(o1, 1, 2), jnp.swapaxes(o3, 1, 2), o2, grad_router

    return jax.shard_map(device_step, mesh=mesh, in_specs=(tok_spec, tok_spec, P(), exp_spec, exp_spec, exp_spec, tok_spec), out_specs=(tok_spec, exp_spec, exp_spec, exp_spec, P()), check_vma=False)
```

```python
import jax
import jax.numpy as jnp
from jax import lax
from jax.experimental import pallas as pl
from jax.experimental.pallas import tpu as pltpu
from jax.sharding import PartitionSpec as P

TILE = 512
GRP = 16
SLOT = 256
NT_DIMS = (((1,), (1,)), ((), ()))
TN_DIMS = (((0,), (0,)), ((), ()))
VMEM = 63 * 2**20
BF = jnp.bfloat16
F32 = jnp.float32


def params(**kw):
    return pltpu.CompilerParams(vmem_limit_bytes=VMEM, **kw)


def cost(flops, nbytes):
    return pl.CostEstimate(flops=int(flops), bytes_accessed=int(nbytes), transcendentals=0)


def pick_rows(slot0, slot1, n_tok):
    row = lax.broadcasted_iota(jnp.int32, (SLOT, n_tok), 0)
    return row == slot0, row == slot1


def gather_rows(order, dst, slot0, slot1, p0, p1, rows_all, n_rows, real, cycle, with_p, into=None):
    n_steps = order.shape[0]
    n_tok = slot0.shape[-1]
    dim = rows_all.shape[1]
    per = SLOT // GRP
    chunk = 1024

    def body(order_ref, dst_ref, s0_ref, s1_ref, p0_ref, p1_ref, x_ref, *rest):
        if into is not None:
            rest = rest[1:]
        if with_p:
            o_ref, po_ref, buf, pbuf, sems, psems = rest
        else:
            o_ref, buf, sems = rest
        i = pl.program_id(0)
        now = lax.rem(i, 2)

        def copies(step, half, j):
            d = dst_ref[step * per + j]
            at = pl.multiple_of(jnp.maximum(d, 0) * GRP, GRP)
            out = [pltpu.make_async_copy(buf.at[half, pl.ds(j * GRP, GRP)], o_ref.at[pl.ds(at, GRP)], sems.at[half, j])]
            if with_p:
                out.append(pltpu.make_async_copy(pbuf.at[half, pl.ds(j * GRP, GRP)], po_ref.at[pl.ds(at, GRP)], psems.at[half, j]))
            return d, out

        def each(step, half, wait):
            for j in range(per):
                d, cs = copies(step, half, j)

                @pl.when(d >= 0)
                def _():
                    for c in cs:
                        if wait:
                            c.wait()
                        else:
                            c.start()

        @pl.when(i >= 2)
        def _():
            each(i - 2, now, True)

        is0, is1 = pick_rows(s0_ref[0], s1_ref[0], n_tok)
        is_real = lax.rem(i, cycle) < real

        @pl.when(is_real)
        def _():
            pick = jnp.where(is0 | is1, 1.0, 0.0).astype(BF)

            @pl.loop(0, dim // chunk)
            def _(c):
                cols = pl.ds(pl.multiple_of(c * chunk, chunk), chunk)
                buf[now, :, cols] = jnp.dot(pick, x_ref[:, cols], preferred_element_type=F32).astype(BF)

        @pl.when(jnp.logical_not(is_real))
        def _():
            buf[now] = jnp.zeros((SLOT, dim), BF)

        if with_p:
            p = jnp.where(is0, p0_ref[0], 0.0) + jnp.where(is1, p1_ref[0], 0.0)
            pbuf[now] = jnp.broadcast_to(jnp.sum(p, axis=1, keepdims=True), (SLOT, 128))
        each(i, now, False)

        @pl.when(i == n_steps - 1)
        def _():
            each(i - 1, 1 - now, True)
            each(i, now, True)

    vec = pl.BlockSpec((1, 1, n_tok), lambda i, o, d: (i, 0, 0))
    outs = [jax.ShapeDtypeStruct((n_rows, dim), BF)]
    scratch = [pltpu.VMEM((2, SLOT, dim), BF), pltpu.SemaphoreType.DMA((2, per))]
    if with_p:
        outs.append(jax.ShapeDtypeStruct((n_rows, 128), F32))
        scratch = [scratch[0], pltpu.VMEM((2, SLOT, 128), F32), scratch[1], pltpu.SemaphoreType.DMA((2, per))]
    return pl.pallas_call(
        body,
        grid_spec=pltpu.PrefetchScalarGridSpec(
            num_scalar_prefetch=2,
            grid=(n_steps,),
            in_specs=[vec, vec, vec, vec, pl.BlockSpec((n_tok, dim), lambda i, o, d: (o[i], 0))]
            + ([] if into is None else [pl.BlockSpec(memory_space=pl.ANY)]),
            out_specs=[pl.BlockSpec(memory_space=pl.ANY)] * len(outs),
            scratch_shapes=scratch,
        ),
        out_shape=outs,
        input_output_aliases={} if into is None else {7: 0},
        compiler_params=params(),
        cost_estimate=cost(2 * n_steps * SLOT * n_tok * dim, rows_all.size * 2 + n_rows * dim * 2),
        name="gather_p" if with_p else "gather_g",
    )(order, dst, slot0, slot1, p0, p1, rows_all, *([] if into is None else [into]))


def forward(tiles, tile_e, n_tiles, xs, w1, w3):
    n_rows, dim = xs.shape
    ff = w1.shape[1]
    nt = tiles.shape[0]

    def body(tl, te, ntr, x_ref, w1_ref, w3_ref, a_ref, u1_ref, u3_ref):
        @pl.when(pl.program_id(0) < ntr[0])
        def _():
            z1 = lax.dot_general(x_ref[...], w1_ref[0], NT_DIMS, preferred_element_type=F32)
            z3 = lax.dot_general(x_ref[...], w3_ref[0], NT_DIMS, preferred_element_type=F32)
            sg = jax.nn.sigmoid(z1)
            s = z1 * sg
            a_ref[...] = (s * z3).astype(BF)
            u1_ref[...] = z3 * sg * (1.0 + z1 * (1.0 - sg))
            u3_ref[...] = s

    at = lambda t, tl, te, n: (tl[t], 0)
    wt = pl.BlockSpec((1, ff, dim), lambda t, tl, te, n: (te[t], 0, 0))
    rf = pl.BlockSpec((TILE, ff), at)
    return pl.pallas_call(
        body,
        grid_spec=pltpu.PrefetchScalarGridSpec(
            num_scalar_prefetch=3,
            grid=(nt,),
            in_specs=[pl.BlockSpec((TILE, dim), at), wt, wt],
            out_specs=[rf, rf, rf],
        ),
        out_shape=[jax.ShapeDtypeStruct((n_rows, ff), d) for d in (BF, F32, F32)],
        compiler_params=params(),
        cost_estimate=cost(4 * n_rows * dim * ff, n_rows * dim * 2),
        name="forward",
    )(tiles, tile_e, n_tiles, xs, w1, w3)


def hidden_grad(tiles, tile_e, n_tiles, gs, ps, a, u1, u3, w2, into=None):
    n_rows, dim = gs.shape
    ff = w2.shape[1]
    nt = tiles.shape[0]
    first = into is None

    def body(tl, te, ntr, g_ref, p_ref, a_ref, u1_ref, u3_ref, w_ref, *rest):
        outs = rest if first else rest[2:]

        @pl.when(pl.program_id(0) < ntr[0])
        def _():
            h = lax.dot_general(g_ref[...], w_ref[0], NT_DIMS, preferred_element_type=F32)
            da = p_ref[:, 0:1] * h
            outs[0][...] = (da * u1_ref[...]).astype(BF)
            outs[1][...] = (da * u3_ref[...]).astype(BF)
            if first:
                q = jnp.sum(a_ref[...].astype(F32) * h, axis=1, keepdims=True)
                outs[2][...] = jnp.broadcast_to(q, outs[2].shape)

    at = lambda t, tl, te, n: (tl[t], 0)
    rf = pl.BlockSpec((TILE, ff), at)
    lane = pl.BlockSpec((TILE, 128), at)
    any_spec = pl.BlockSpec(memory_space=pl.ANY)
    return pl.pallas_call(
        body,
        grid_spec=pltpu.PrefetchScalarGridSpec(
            num_scalar_prefetch=3,
            grid=(nt,),
            in_specs=[pl.BlockSpec((TILE, dim), at), lane, rf, rf, rf, pl.BlockSpec((1, ff, dim), lambda t, tl, te, n: (te[t], 0, 0))]
            + ([] if first else [any_spec, any_spec]),
            out_specs=[rf, rf] + ([lane] if first else []),
        ),
        out_shape=[jax.ShapeDtypeStruct((n_rows, ff), BF)] * 2 + ([jax.ShapeDtypeStruct((n_rows, 128), F32)] if first else []),
        input_output_aliases={} if first else {9: 0, 10: 1},
        compiler_params=params(),
        cost_estimate=cost(2 * nt * TILE * dim * ff, nt * TILE * dim * 2),
        name="hidden_grad",
    )(tiles, tile_e, n_tiles, gs, ps, a, u1, u3, w2, *(into or []))


def row_grad(tiles, tiles_e, n_tiles, inverse, d1, d3, w1, w3, n_out, first, width):
    ff = d1.shape[1]
    nl = tiles.shape[0]
    per = TILE // GRP
    chunk = min(width, 1024)

    def body(tl, te, ntr, inv, d1_ref, d3_ref, w1_ref, w3_ref, o_ref, buf, sems):
        t = pl.program_id(0)
        now = lax.rem(t, 2)

        def each(step, half, wait):
            for j in range(per):
                d = inv[tl[step] * per + j]
                at = pl.multiple_of(jnp.maximum(d, 0) * GRP, GRP)

                @pl.when((step < ntr[0]) & (d >= 0))
                def _():
                    c = pltpu.make_async_copy(buf.at[half, pl.ds(j * GRP, GRP)], o_ref.at[pl.ds(at, GRP)], sems.at[half, j])
                    if wait:
                        c.wait()
                    else:
                        c.start()

        @pl.when(t >= 2)
        def _():
            each(t - 2, now, True)

        @pl.when(t < ntr[0])
        def _():
            for c in range(width // chunk):
                cols = pl.ds(c * chunk, chunk)
                r = jnp.dot(d1_ref[...], w1_ref[0, :, cols], preferred_element_type=F32)
                r += jnp.dot(d3_ref[...], w3_ref[0, :, cols], preferred_element_type=F32)
                buf[now, :, cols] = r.astype(BF)

        each(t, now, False)

        @pl.when(t == nl - 1)
        def _():
            each(t - 1, 1 - now, True)
            each(t, now, True)

    at = pl.BlockSpec((TILE, ff), lambda t, tl, te, n, inv: (tl[t], 0))
    wt = pl.BlockSpec((1, ff, width), lambda t, tl, te, n, inv: (te[t], 0, first // width))
    return pl.pallas_call(
        body,
        grid_spec=pltpu.PrefetchScalarGridSpec(
            num_scalar_prefetch=4,
            grid=(nl,),
            in_specs=[at, at, wt, wt],
            out_specs=pl.BlockSpec(memory_space=pl.ANY),
            scratch_shapes=[pltpu.VMEM((2, TILE, width), BF), pltpu.SemaphoreType.DMA((2, per))],
        ),
        out_shape=jax.ShapeDtypeStruct((n_out, width), BF),
        compiler_params=params(),
        cost_estimate=cost(4 * nl * TILE * width * ff, n_out * width * 2),
        name="row_grad",
    )(tiles, tiles_e, n_tiles, inverse, d1, d3, w1, w3)


def weight_grads(tiles, tile_e, n_tiles, xs, gs, ps, a, d1, d3):
    n_rows, dim = xs.shape
    ff = a.shape[1]
    nt = tiles.shape[0]
    cols = 2048
    chunk = 512

    def body(tl, te, ntr, x_ref, g_ref, p_ref, a_ref, d1_ref, d3_ref, o1_ref, o3_ref, o2_ref):
        t = pl.program_id(1)
        fresh = (t == 0) | (te[t] != te[jnp.maximum(t - 1, 0)])

        def add(start):
            a_t, d1_t, d3_t = (r[...].T for r in (a_ref, d1_ref, d3_ref))

            def put(out, at, lhs_t, rhs):
                new = jnp.dot(lhs_t, rhs, preferred_element_type=F32)
                out[0, :, at] = new if start else out[0, :, at] + new

            @pl.loop(0, cols // chunk)
            def _(c):
                at = pl.ds(pl.multiple_of(c * chunk, chunk), chunk)
                x = x_ref[:, at]
                put(o1_ref, at, d1_t, x)
                put(o3_ref, at, d3_t, x)
                put(o2_ref, at, a_t, (p_ref[:, 0:1] * g_ref[:, at].astype(F32)).astype(BF))

        @pl.when((t < ntr[0]) & fresh)
        def _():
            add(True)

        @pl.when((t < ntr[0]) & jnp.logical_not(fresh))
        def _():
            add(False)

    wide = pl.BlockSpec((TILE, cols), lambda d, t, tl, te, n: (tl[t], d))
    rf = pl.BlockSpec((TILE, ff), lambda d, t, tl, te, n: (tl[t], 0))
    lane = pl.BlockSpec((TILE, 128), lambda d, t, tl, te, n: (tl[t], 0))
    out = pl.BlockSpec((1, ff, cols), lambda d, t, tl, te, n: (te[t], 0, d))
    return pl.pallas_call(
        body,
        grid_spec=pltpu.PrefetchScalarGridSpec(
            num_scalar_prefetch=3,
            grid=(dim // cols, nt),
            in_specs=[wide, wide, lane, rf, rf, rf],
            out_specs=[out, out, out],
        ),
        out_shape=[jax.ShapeDtypeStruct((2, ff, dim), F32)] * 3,
        compiler_params=params(),
        cost_estimate=cost(6 * n_rows * dim * ff, 4 * n_rows * dim + 12 * ff * dim * 2),
        name="weight_grads",
    )(tiles, tile_e, n_tiles, xs, gs, ps, a, d1, d3)


def combine(valid, i0, i1, dl, wr_t, blocks):
    n_tok = i0.shape[0]
    dim = wr_t.shape[1]
    n_src = len(blocks[0])
    width = blocks[0][0].shape[1]
    cols = 512
    per = width // cols
    n_half = len(blocks)

    def body(nv, i0_ref, i1_ref, dl_ref, w_ref, *rest):
        refs, o_ref, pick = rest[: n_src * n_half], rest[-2], rest[-1]
        c = pl.program_id(0)

        @pl.when(c == 0)
        def _():
            col = lax.broadcasted_iota(jnp.int32, (n_tok, n_src * SLOT), 1)
            pick[...] = jnp.where((col == i0_ref[...]) | (col == i1_ref[...]), 1.0, 0.0).astype(BF)

        for h in range(n_half):

            @pl.when((c >= h * per) & (c < (h + 1) * per))
            def _():
                acc = jnp.dot(dl_ref[...], w_ref[...], preferred_element_type=F32)
                row = lax.broadcasted_iota(jnp.int32, (SLOT, cols), 0)
                tot = jnp.zeros((n_tok, cols), F32)
                for b in range(n_src):
                    blk = jnp.where(row < nv[b], refs[h * n_src + b][...].astype(F32), 0.0).astype(BF)
                    tot += jnp.dot(pick[:, b * SLOT : (b + 1) * SLOT], blk, preferred_element_type=F32)
                o_ref[...] = (tot + acc).astype(BF)

    one = pl.BlockSpec((n_tok, 1), lambda c, nv: (0, 0))
    ins = [one, one, pl.BlockSpec((n_tok, dl.shape[1]), lambda c, nv: (0, 0)), pl.BlockSpec((dl.shape[1], cols), lambda c, nv: (0, c))]
    for h in range(n_half):
        ins += [pl.BlockSpec((SLOT, cols), lambda c, nv, h=h: (0, jnp.clip(c - h * per, 0, per - 1)))] * n_src
    return pl.pallas_call(
        body,
        grid_spec=pltpu.PrefetchScalarGridSpec(
            num_scalar_prefetch=1,
            grid=(dim // cols,),
            in_specs=ins,
            out_specs=pl.BlockSpec((n_tok, cols), lambda c, nv: (0, c)),
            scratch_shapes=[pltpu.VMEM((n_tok, n_src * SLOT), BF)],
        ),
        out_shape=jax.ShapeDtypeStruct((n_tok, dim), BF),
        compiler_params=params(),
        cost_estimate=cost(2 * n_tok * n_src * SLOT * dim, n_src * SLOT * dim * 2),
        name="combine",
    )(valid, i0, i1, dl, wr_t, *[b for half in blocks for b in half])


def up(v, m):
    return (v + m - 1) // m * m


def before(v):
    i = jnp.arange(v.shape[-1], dtype=jnp.int32)
    return jnp.sum(jnp.where(i[None, None, :] < i[None, :, None], v[:, None, :], 0), axis=2)


def running(mask):
    n = mask.shape[-1]
    i = jnp.arange(n, dtype=jnp.int32)
    tri = (i[:, None] <= i[None, :]).astype(BF)
    return jnp.dot(mask.astype(BF), tri, preferred_element_type=F32).astype(jnp.int32)


def solution(mesh):
    n_dp, n_ep = mesh.shape["dp"], mesh.shape["ep"]
    tok_spec = P(("dp", "ep"), None)
    exp_spec = P("ep", None, None)
    both = ("dp", "ep")

    def device_step(x_loc, route_idx, w_router, w_gate, w_up, w_down, g_loc):
        n_tok, top_k = route_idx.shape
        dim = x_loc.shape[1]
        n_exp = w_router.shape[1]
        my_dp, my_ep = lax.axis_index("dp"), lax.axis_index("ep")
        n_sh = n_dp * n_ep
        per = SLOT // GRP
        fill = TILE // GRP
        n_half = n_dp
        half_t = n_ep * SLOT // TILE + 1
        n_rows = n_half * half_t * TILE
        i32 = jnp.int32

        x_all = lax.all_gather(x_loc, both, axis=0, tiled=True)
        g_all = lax.all_gather(g_loc, both, axis=0, tiled=True)

        w1 = jnp.swapaxes(w_gate, 1, 2)
        w3 = jnp.swapaxes(w_up, 1, 2)
        wr_t = w_router.T

        logits = lax.dot_general(wr_t, x_loc, NT_DIMS, preferred_element_type=F32)
        idx = route_idx.T
        eid = jnp.arange(n_exp, dtype=i32)
        hot = [idx[k][None, :] == eid[:, None] for k in range(top_k)]
        sel = jnp.stack([jnp.sum(jnp.where(h, logits, 0.0), axis=0) for h in hot])
        probs = jax.nn.softmax(sel, axis=0)
        meta = lax.all_gather(jnp.concatenate([idx.astype(F32), probs]), both, axis=0)

        step = jnp.arange(n_sh, dtype=i32)
        order = ((my_dp + step // n_ep) % n_dp) * n_ep + ((step % n_ep) ^ my_ep)
        meta = meta[order]
        i_all, p_all = meta[:, :top_k].astype(i32), meta[:, top_k:]
        e0 = my_ep * 2
        m0 = [i_all[:, k] == e0 for k in range(top_k)]
        m1 = [i_all[:, k] == e0 + 1 for k in range(top_k)]
        m0, m1, p0, p1 = m0[0] | m0[1], m1[0] | m1[1], jnp.where(m0[0], p_all[:, 0], p_all[:, 1]), jnp.where(m1[0], p_all[:, 0], p_all[:, 1])
        run = running(jnp.concatenate([m0, m1]))
        r0, r1 = run[:n_sh], run[n_sh:]
        k0, k1 = up(r0[:, -1], GRP) // GRP, up(r1[:, -1], GRP) // GRP
        slot0 = jnp.where(m0, r0 - 1, -1)
        slot1 = jnp.where(m1, k0[:, None] * GRP + r1 - 1, -1)
        h0, h1 = k0.reshape(n_half, n_ep), k1.reshape(n_half, n_ep)
        t0, t1 = jnp.sum(h0, axis=1), jnp.sum(h1, axis=1)
        n0, n1 = up(t0, fill) // fill, up(t1, fill) // fill
        base = jnp.arange(n_half, dtype=i32) * (half_t * fill)
        s0 = (base[:, None] + before(h0)).reshape(-1)
        s1 = ((base + n0 * fill)[:, None] + before(h1)).reshape(-1)
        j = jnp.arange(per, dtype=i32)[None, :]
        dst = jnp.where(j < k0[:, None], s0[:, None] + j, jnp.where(j < (k0 + k1)[:, None], s1[:, None] + j - k0[:, None], -1))
        f = jnp.arange(fill, dtype=i32)[None, :]
        gap0 = jnp.where(t0[:, None] + f < (n0 * fill)[:, None], (base + t0)[:, None] + f, -1)
        gap1 = jnp.where(t1[:, None] + f < (n1 * fill)[:, None], (base + n0 * fill + t1)[:, None] + f, -1)
        dst_all = jnp.concatenate([dst.reshape(n_half, -1), gap0, gap1], axis=1).reshape(-1)
        n_fill = 2 * fill // per
        cycle = n_ep + n_fill
        order_h = order.reshape(n_half, n_ep)
        order_all = jnp.concatenate([order_h, jnp.broadcast_to(order_h[:, -1:], (n_half, n_fill))], axis=1).reshape(-1)

        def pad(v, c):
            v = jnp.concatenate([v.reshape(n_half, n_ep, n_tok), jnp.full((n_half, n_fill, n_tok), c, v.dtype)], axis=1)
            return v.reshape(n_half * cycle, 1, n_tok)

        slot0, slot1, p0, p1 = pad(slot0, -1), pad(slot1, -1), pad(p0, 0.0), pad(p1, 0.0)

        na, nb, nc, nd = n0[0], n0[1], n1[0], n1[1]
        total = na + nb + nc + nd
        t = jnp.minimum(jnp.arange(n_half * half_t, dtype=i32), total - 1)
        all_t = jnp.where(t < na, t, jnp.where(t < na + nb, half_t + t - na, jnp.where(t < na + nb + nc, t - nb, half_t + t - na - nc)))
        all_l = (all_t, (t >= na + nb).astype(i32), total[None])
        t = jnp.arange(half_t, dtype=i32)
        tl, to = jnp.minimum(t, na + nc - 1), jnp.minimum(t, nb + nd - 1)
        own_l = (tl, (tl >= na).astype(i32), (na + nc)[None])
        oth_l = (half_t + to, (to >= nb).astype(i32), (nb + nd)[None])

        dst_loc = dst[:n_ep]
        grp = jnp.arange(half_t * fill, dtype=i32)
        inverse = jnp.sum(jnp.where(dst_loc.reshape(-1)[:, None] == grp[None, :], jnp.arange(n_ep * per, dtype=i32)[:, None] + 1, 0), axis=0) - 1

        mine = jnp.concatenate(hot)
        rank = running(mine)
        cnt = rank[:n_exp] + rank[n_exp:]
        kk = up(cnt[:, -1], GRP)
        off = jnp.where(eid % 2 == 1, jnp.concatenate([kk[:1], kk[:-1]]), 0)
        slot = off[:, None] + cnt - 1
        own = [jnp.sum(jnp.where(h, slot, 0), axis=0) for h in hot]
        src = [idx[k] // 2 for k in range(top_k)]
        nat = [src[k] * SLOT + own[k] for k in range(top_k)]
        ret = [((src[k] ^ my_ep) * SLOT + own[k])[:, None] for k in range(top_k)]
        dev = jnp.arange(n_ep, dtype=i32)
        full = kk.reshape(n_ep, 2).sum(axis=1)
        valid = jnp.sum(jnp.where((dev ^ my_ep)[:, None] == dev[None, :], full[None, :], 0), axis=1)

        tabs = (order_all, dst_all, slot0, slot1, p0, p1)
        cut = lambda h: [v[h * (v.shape[0] // n_half) : (h + 1) * (v.shape[0] // n_half)] for v in tabs]
        xs, ps = gather_rows(*tabs, x_all, n_rows, n_ep, cycle, True)
        a, u1, u3 = forward(*all_l, xs, w1, w3)

        (gs,) = gather_rows(*cut(0), g_all, n_rows, n_ep, cycle, False)
        d1, d3, q = hidden_grad(*own_l, gs, ps, a, u1, u3, w_down)

        nat_dst = dst_loc[dev ^ my_ep].reshape(-1)
        q_send = q[: half_t * TILE, 0].reshape(half_t * fill, GRP)[jnp.maximum(nat_dst, 0)].reshape(n_ep, SLOT)
        q_recv = lax.all_to_all(q_send, "ep", 0, 0, tiled=True).reshape(1, n_ep * SLOT)
        spot = jnp.arange(n_ep * SLOT, dtype=i32)[None, :]
        qk = [jnp.sum(jnp.where(spot == nat[k][:, None], q_recv, 0.0), axis=1) for k in range(top_k)]
        mean = probs[0] * qk[0] + probs[1] * qk[1]
        dl = [probs[k] * (qk[k] - mean) for k in range(top_k)]
        d_logits = sum(jnp.where(idx[k][:, None] == eid[None, :], dl[k][:, None], 0.0) for k in range(top_k)).astype(BF)
        part_router = lax.dot_general(d_logits, x_loc, TN_DIMS, preferred_element_type=F32)
        grad_router = lax.psum(part_router, both).T

        n_cut = 2
        width = dim // n_cut
        blocks = []
        d1r, d3r = d1, d3
        for c in range(n_cut):
            rows = row_grad(*own_l, inverse, d1r, d3r, w1, w3, n_ep * SLOT, c * width, width)
            parts = [rows[b * SLOT : (b + 1) * SLOT] for b in range(n_ep)]
            d1r, d3r, *parts = lax.optimization_barrier((d1r, d3r, *parts))
            blocks.append(parts[:1] + [lax.ppermute(parts[b], "ep", [(s, s ^ b) for s in range(n_ep)]) for b in range(1, n_ep)])

        gs, d1, d3, _ = lax.optimization_barrier((gs, d1r, d3r, part_router))
        (gs,) = gather_rows(*cut(1), g_all, n_rows, n_ep, cycle, False, into=gs)
        d1, d3 = hidden_grad(*oth_l, gs, ps, a, u1, u3, w_down, into=[d1, d3])
        o1, o3, o2 = weight_grads(*all_l, xs, gs, ps, a, d1, d3)
        grad_x = combine(valid, ret[0], ret[1], d_logits, wr_t, blocks)
        return grad_x, jnp.swapaxes(o1, 1, 2), jnp.swapaxes(o3, 1, 2), o2, grad_router

    return jax.shard_map(device_step, mesh=mesh, in_specs=(tok_spec, tok_spec, P(), exp_spec, exp_spec, exp_spec, tok_spec), out_specs=(tok_spec, exp_spec, exp_spec, exp_spec, P()), check_vma=False)
```

```python
import jax
import jax.numpy as jnp
from jax import lax
from jax.experimental import pallas as pl
from jax.experimental.pallas import tpu as pltpu
from jax.sharding import PartitionSpec as P

TILE = 512
GRP = 16
SLOT = 256
BASE = 128
MORE = 64
NT_DIMS = (((1,), (1,)), ((), ()))
TN_DIMS = (((0,), (0,)), ((), ()))
VMEM = 63 * 2**20
BF = jnp.bfloat16
F32 = jnp.float32


def params(**kw):
    return pltpu.CompilerParams(vmem_limit_bytes=VMEM, **kw)


def cost(flops, nbytes):
    return pl.CostEstimate(flops=int(flops), bytes_accessed=int(nbytes), transcendentals=0)


def pick_rows(slot0, slot1, n_tok):
    row = lax.broadcasted_iota(jnp.int32, (SLOT, n_tok), 0)
    return row == slot0, row == slot1


def gather_rows(order, dst, slot0, slot1, p0, p1, rows_all, n_rows, real, cycle, with_p, into=None):
    n_steps = order.shape[0]
    n_tok = slot0.shape[-1]
    dim = rows_all.shape[1]
    per = SLOT // GRP
    chunk = 1024

    def body(order_ref, dst_ref, s0_ref, s1_ref, p0_ref, p1_ref, x_ref, *rest):
        if into is not None:
            rest = rest[1:]
        if with_p:
            o_ref, po_ref, buf, pbuf, sems, psems = rest
        else:
            o_ref, buf, sems = rest
        i = pl.program_id(0)
        now = lax.rem(i, 2)

        def copies(step, half, j):
            d = dst_ref[step * per + j]
            at = pl.multiple_of(jnp.maximum(d, 0) * GRP, GRP)
            out = [pltpu.make_async_copy(buf.at[half, pl.ds(j * GRP, GRP)], o_ref.at[pl.ds(at, GRP)], sems.at[half, j])]
            if with_p:
                out.append(pltpu.make_async_copy(pbuf.at[half, pl.ds(j * GRP, GRP)], po_ref.at[pl.ds(at, GRP)], psems.at[half, j]))
            return d, out

        def each(step, half, wait):
            for j in range(per):
                d, cs = copies(step, half, j)

                @pl.when(d >= 0)
                def _():
                    for c in cs:
                        if wait:
                            c.wait()
                        else:
                            c.start()

        @pl.when(i >= 2)
        def _():
            each(i - 2, now, True)

        is0, is1 = pick_rows(s0_ref[0], s1_ref[0], n_tok)
        is_real = lax.rem(i, cycle) < real

        @pl.when(is_real)
        def _():
            pick = jnp.where(is0 | is1, 1.0, 0.0).astype(BF)

            @pl.loop(0, dim // chunk)
            def _(c):
                cols = pl.ds(pl.multiple_of(c * chunk, chunk), chunk)
                buf[now, :, cols] = jnp.dot(pick, x_ref[:, cols], preferred_element_type=F32).astype(BF)

        @pl.when(jnp.logical_not(is_real))
        def _():
            buf[now] = jnp.zeros((SLOT, dim), BF)

        if with_p:
            p = jnp.where(is0, p0_ref[0], 0.0) + jnp.where(is1, p1_ref[0], 0.0)
            pbuf[now] = jnp.broadcast_to(jnp.sum(p, axis=1, keepdims=True), (SLOT, 128))
        each(i, now, False)

        @pl.when(i == n_steps - 1)
        def _():
            each(i - 1, 1 - now, True)
            each(i, now, True)

    vec = pl.BlockSpec((1, 1, n_tok), lambda i, o, d: (i, 0, 0))
    outs = [jax.ShapeDtypeStruct((n_rows, dim), BF)]
    scratch = [pltpu.VMEM((2, SLOT, dim), BF), pltpu.SemaphoreType.DMA((2, per))]
    if with_p:
        outs.append(jax.ShapeDtypeStruct((n_rows, 128), F32))
        scratch = [scratch[0], pltpu.VMEM((2, SLOT, 128), F32), scratch[1], pltpu.SemaphoreType.DMA((2, per))]
    return pl.pallas_call(
        body,
        grid_spec=pltpu.PrefetchScalarGridSpec(
            num_scalar_prefetch=2,
            grid=(n_steps,),
            in_specs=[vec, vec, vec, vec, pl.BlockSpec((n_tok, dim), lambda i, o, d: (o[i], 0))]
            + ([] if into is None else [pl.BlockSpec(memory_space=pl.ANY)]),
            out_specs=[pl.BlockSpec(memory_space=pl.ANY)] * len(outs),
            scratch_shapes=scratch,
        ),
        out_shape=outs,
        input_output_aliases={} if into is None else {7: 0},
        compiler_params=params(),
        cost_estimate=cost(2 * n_steps * SLOT * n_tok * dim, rows_all.size * 2 + n_rows * dim * 2),
        name="gather_p" if with_p else "gather_g",
    )(order, dst, slot0, slot1, p0, p1, rows_all, *([] if into is None else [into]))


def forward(tiles, tile_e, n_tiles, xs, w1, w3):
    n_rows, dim = xs.shape
    ff = w1.shape[1]
    nt = tiles.shape[0]

    def body(tl, te, ntr, x_ref, w1_ref, w3_ref, a_ref, at_ref, u1_ref, u3_ref):
        @pl.when(pl.program_id(0) < ntr[0])
        def _():
            z1 = lax.dot_general(x_ref[...], w1_ref[0], NT_DIMS, preferred_element_type=F32)
            z3 = lax.dot_general(x_ref[...], w3_ref[0], NT_DIMS, preferred_element_type=F32)
            sg = jax.nn.sigmoid(z1)
            s = z1 * sg
            a_ref[...] = (s * z3).astype(BF)
            at_ref[...] = a_ref[...].T
            u1_ref[...] = z3 * sg * (1.0 + z1 * (1.0 - sg))
            u3_ref[...] = s

    at = lambda t, tl, te, n: (tl[t], 0)
    wt = pl.BlockSpec((1, ff, dim), lambda t, tl, te, n: (te[t], 0, 0))
    rf = pl.BlockSpec((TILE, ff), at)
    return pl.pallas_call(
        body,
        grid_spec=pltpu.PrefetchScalarGridSpec(
            num_scalar_prefetch=3,
            grid=(nt,),
            in_specs=[pl.BlockSpec((TILE, dim), at), wt, wt],
            out_specs=[rf, pl.BlockSpec((ff, TILE), lambda t, tl, te, n: (0, tl[t])), rf, rf],
        ),
        out_shape=[jax.ShapeDtypeStruct(sh, d) for sh, d in (((n_rows, ff), BF), ((ff, n_rows), BF), ((n_rows, ff), F32), ((n_rows, ff), F32))],
        compiler_params=params(),
        cost_estimate=cost(4 * n_rows * dim * ff, n_rows * dim * 2),
        name="forward",
    )(tiles, tile_e, n_tiles, xs, w1, w3)


def hidden_grad(tiles, tile_e, n_tiles, gs, ps, a, u1, u3, w2, into=None):
    n_rows, dim = gs.shape
    ff = w2.shape[1]
    nt = tiles.shape[0]
    first = into is None

    def body(tl, te, ntr, g_ref, p_ref, a_ref, u1_ref, u3_ref, w_ref, *rest):
        outs = rest if first else rest[2:]

        @pl.when(pl.program_id(0) < ntr[0])
        def _():
            h = lax.dot_general(g_ref[...], w_ref[0], NT_DIMS, preferred_element_type=F32)
            da = p_ref[:, 0:1] * h
            d1 = (da * u1_ref[...]).astype(BF)
            d3 = (da * u3_ref[...]).astype(BF)
            outs[0][...] = d1.T
            outs[1][...] = d3.T
            if first:
                outs[2][...] = d1
                outs[3][...] = d3
                q = jnp.sum(a_ref[...].astype(F32) * h, axis=1, keepdims=True)
                outs[4][...] = jnp.broadcast_to(q, outs[4].shape)

    at = lambda t, tl, te, n: (tl[t], 0)
    rf = pl.BlockSpec((TILE, ff), at)
    lane = pl.BlockSpec((TILE, 128), at)
    turned = pl.BlockSpec((ff, TILE), lambda t, tl, te, n: (0, tl[t]))
    any_spec = pl.BlockSpec(memory_space=pl.ANY)
    return pl.pallas_call(
        body,
        grid_spec=pltpu.PrefetchScalarGridSpec(
            num_scalar_prefetch=3,
            grid=(nt,),
            in_specs=[pl.BlockSpec((TILE, dim), at), lane, rf, rf, rf, pl.BlockSpec((1, ff, dim), lambda t, tl, te, n: (te[t], 0, 0))]
            + ([] if first else [any_spec, any_spec]),
            out_specs=[turned, turned] + ([rf, rf, lane] if first else []),
        ),
        out_shape=[jax.ShapeDtypeStruct((ff, n_rows), BF)] * 2
        + ([jax.ShapeDtypeStruct((n_rows, ff), BF)] * 2 + [jax.ShapeDtypeStruct((n_rows, 128), F32)] if first else []),
        input_output_aliases={} if first else {9: 0, 10: 1},
        compiler_params=params(),
        cost_estimate=cost(2 * nt * TILE * dim * ff, nt * TILE * dim * 2),
        name="hidden_grad",
    )(tiles, tile_e, n_tiles, gs, ps, a, u1, u3, w2, *(into or []))


def row_grad(tiles, tiles_e, n_tiles, inverse, d1, d3, w1, w3, n_out, first, width):
    ff = d1.shape[1]
    nl = tiles.shape[0]
    per = TILE // GRP
    chunk = min(width, 1024)

    def body(tl, te, ntr, inv, d1_ref, d3_ref, w1_ref, w3_ref, o_ref, buf, sems):
        t = pl.program_id(0)
        now = lax.rem(t, 2)

        def each(step, half, wait):
            for j in range(per):
                d = inv[tl[step] * per + j]
                at = pl.multiple_of(jnp.maximum(d, 0) * GRP, GRP)

                @pl.when((step < ntr[0]) & (d >= 0))
                def _():
                    c = pltpu.make_async_copy(buf.at[half, pl.ds(j * GRP, GRP)], o_ref.at[pl.ds(at, GRP)], sems.at[half, j])
                    if wait:
                        c.wait()
                    else:
                        c.start()

        @pl.when(t >= 2)
        def _():
            each(t - 2, now, True)

        @pl.when(t < ntr[0])
        def _():
            for c in range(width // chunk):
                cols = pl.ds(c * chunk, chunk)
                r = jnp.dot(d1_ref[...], w1_ref[0, :, cols], preferred_element_type=F32)
                r += jnp.dot(d3_ref[...], w3_ref[0, :, cols], preferred_element_type=F32)
                buf[now, :, cols] = r.astype(BF)

        each(t, now, False)

        @pl.when(t == nl - 1)
        def _():
            each(t - 1, 1 - now, True)
            each(t, now, True)

    at = pl.BlockSpec((TILE, ff), lambda t, tl, te, n, inv: (tl[t], 0))
    wt = pl.BlockSpec((1, ff, width), lambda t, tl, te, n, inv: (te[t], 0, first // width))
    return pl.pallas_call(
        body,
        grid_spec=pltpu.PrefetchScalarGridSpec(
            num_scalar_prefetch=4,
            grid=(nl,),
            in_specs=[at, at, wt, wt],
            out_specs=pl.BlockSpec(memory_space=pl.ANY),
            scratch_shapes=[pltpu.VMEM((2, TILE, width), BF), pltpu.SemaphoreType.DMA((2, per))],
        ),
        out_shape=jax.ShapeDtypeStruct((n_out, width), BF),
        compiler_params=params(),
        cost_estimate=cost(4 * nl * TILE * width * ff, n_out * width * 2),
        name="row_grad",
    )(tiles, tiles_e, n_tiles, inverse, d1, d3, w1, w3)


def weight_grads(tiles, tile_e, n_tiles, xs, gs, ps, a_t, d1_t, d3_t):
    n_rows, dim = xs.shape
    ff = a_t.shape[0]
    nt = tiles.shape[0]
    cols = 2048
    chunk = 512

    def body(tl, te, ntr, x_ref, g_ref, p_ref, a_ref, d1_ref, d3_ref, *outs):
        t = pl.program_id(1)
        fresh = (t == 0) | (te[t] != te[jnp.maximum(t - 1, 0)])

        def add(start):
            def put(k, at, lhs_t, rhs):
                out = outs[k]
                new = jnp.dot(lhs_t[...], rhs, preferred_element_type=F32)
                if not start:
                    new += out[0, :, at]
                out[0, :, at] = new

            @pl.loop(0, cols // chunk)
            def _(c):
                at = pl.ds(pl.multiple_of(c * chunk, chunk), chunk)
                x = x_ref[:, at]
                put(0, at, d1_ref, x)
                put(1, at, d3_ref, x)
                put(2, at, a_ref, (p_ref[:, 0:1] * g_ref[:, at].astype(F32)).astype(BF))

        @pl.when((t < ntr[0]) & fresh)
        def _():
            add(True)

        @pl.when((t < ntr[0]) & jnp.logical_not(fresh))
        def _():
            add(False)

    wide = pl.BlockSpec((TILE, cols), lambda d, t, tl, te, n: (tl[t], d))
    rf = pl.BlockSpec((ff, TILE), lambda d, t, tl, te, n: (0, tl[t]))
    lane = pl.BlockSpec((TILE, 128), lambda d, t, tl, te, n: (tl[t], 0))
    out = pl.BlockSpec((1, ff, cols), lambda d, t, tl, te, n: (te[t], 0, d))
    return pl.pallas_call(
        body,
        grid_spec=pltpu.PrefetchScalarGridSpec(
            num_scalar_prefetch=3,
            grid=(dim // cols, nt),
            in_specs=[wide, wide, lane, rf, rf, rf],
            out_specs=[out, out, out],
        ),
        out_shape=[jax.ShapeDtypeStruct((2, ff, dim), F32)] * 3,
        compiler_params=params(),
        cost_estimate=cost(6 * nt * TILE * dim * ff, 4 * n_rows * dim + 12 * ff * dim * 2),
        name="weight_grads",
    )(tiles, tile_e, n_tiles, xs, gs, ps, a_t, d1_t, d3_t)


def combine(valid, i0, i1, dl, wr_t, blocks):
    n_tok = i0.shape[0]
    dim = wr_t.shape[1]
    sizes = [b.shape[0] for b in blocks]
    total = sum(sizes)
    cols = 512

    def body(nv, i0_ref, i1_ref, dl_ref, w_ref, *rest):
        refs, o_ref, pick, rows = rest[:-3], rest[-3], rest[-2], rest[-1]

        @pl.when(pl.program_id(0) == 0)
        def _():
            col = lax.broadcasted_iota(jnp.int32, (n_tok, total), 1)
            pick[...] = jnp.where((col == i0_ref[...]) | (col == i1_ref[...]), 1.0, 0.0).astype(BF)

        at = 0
        for b, size in enumerate(sizes):
            row = lax.broadcasted_iota(jnp.int32, (size, cols), 0)
            rows[at : at + size] = jnp.where(row < nv[b], refs[b][...].astype(F32), 0.0).astype(BF)
            at += size
        tot = jnp.dot(pick[...], rows[...], preferred_element_type=F32)
        o_ref[...] = (tot + jnp.dot(dl_ref[...], w_ref[...], preferred_element_type=F32)).astype(BF)

    one = pl.BlockSpec((n_tok, 1), lambda c, nv: (0, 0))
    ins = [one, one, pl.BlockSpec((n_tok, dl.shape[1]), lambda c, nv: (0, 0)), pl.BlockSpec((dl.shape[1], cols), lambda c, nv: (0, c))]
    ins += [pl.BlockSpec((size, cols), lambda c, nv: (0, c)) for size in sizes]
    return pl.pallas_call(
        body,
        grid_spec=pltpu.PrefetchScalarGridSpec(
            num_scalar_prefetch=1,
            grid=(dim // cols,),
            in_specs=ins,
            out_specs=pl.BlockSpec((n_tok, cols), lambda c, nv: (0, c)),
            scratch_shapes=[pltpu.VMEM((n_tok, total), BF), pltpu.VMEM((total, cols), BF)],
        ),
        out_shape=jax.ShapeDtypeStruct((n_tok, dim), BF),
        compiler_params=params(),
        cost_estimate=cost(2 * n_tok * total * dim, total * dim * 2),
        name="combine",
    )(valid, i0, i1, dl, wr_t, *blocks)


def up(v, m):
    return (v + m - 1) // m * m


def before(v):
    i = jnp.arange(v.shape[-1], dtype=jnp.int32)
    return jnp.sum(jnp.where(i[None, None, :] < i[None, :, None], v[:, None, :], 0), axis=2)


def running(mask):
    n = mask.shape[-1]
    i = jnp.arange(n, dtype=jnp.int32)
    tri = (i[:, None] <= i[None, :]).astype(BF)
    return jnp.dot(mask.astype(BF), tri, preferred_element_type=F32).astype(jnp.int32)


def solution(mesh):
    n_dp, n_ep = mesh.shape["dp"], mesh.shape["ep"]
    tok_spec = P(("dp", "ep"), None)
    exp_spec = P("ep", None, None)
    both = ("dp", "ep")

    def device_step(x_loc, route_idx, w_router, w_gate, w_up, w_down, g_loc):
        n_tok, top_k = route_idx.shape
        dim = x_loc.shape[1]
        n_exp = w_router.shape[1]
        my_dp, my_ep = lax.axis_index("dp"), lax.axis_index("ep")
        n_sh = n_dp * n_ep
        per = SLOT // GRP
        fill = TILE // GRP
        n_half = n_dp
        half_t = n_ep * SLOT // TILE + 1
        n_rows = n_half * half_t * TILE
        i32 = jnp.int32

        x_all = lax.all_gather(x_loc, both, axis=0, tiled=True)

        w1 = jnp.swapaxes(w_gate, 1, 2)
        w3 = jnp.swapaxes(w_up, 1, 2)
        wr_t = w_router.T

        logits = lax.dot_general(wr_t, x_loc, NT_DIMS, preferred_element_type=F32)
        idx = route_idx.T
        eid = jnp.arange(n_exp, dtype=i32)
        hot = [idx[k][None, :] == eid[:, None] for k in range(top_k)]
        sel = jnp.stack([jnp.sum(jnp.where(h, logits, 0.0), axis=0) for h in hot])
        probs = jax.nn.softmax(sel, axis=0)
        meta = lax.all_gather(jnp.concatenate([idx.astype(F32), probs]), both, axis=0)

        g_in, meta = lax.optimization_barrier((g_loc, meta))
        g_own = lax.all_gather(g_in, "ep", axis=0, tiled=True)
        g_out, x_all = lax.optimization_barrier((g_loc, x_all))
        g_far = lax.ppermute(g_out, "dp", [(s, (s + 1) % n_dp) for s in range(n_dp)])

        step = jnp.arange(n_sh, dtype=i32)
        order = ((my_dp + step // n_ep) % n_dp) * n_ep + ((step % n_ep) ^ my_ep)
        meta = meta[order]
        i_all, p_all = meta[:, :top_k].astype(i32), meta[:, top_k:]
        e0 = my_ep * 2
        m0 = [i_all[:, k] == e0 for k in range(top_k)]
        m1 = [i_all[:, k] == e0 + 1 for k in range(top_k)]
        m0, m1, p0, p1 = m0[0] | m0[1], m1[0] | m1[1], jnp.where(m0[0], p_all[:, 0], p_all[:, 1]), jnp.where(m1[0], p_all[:, 0], p_all[:, 1])
        run = running(jnp.concatenate([m0, m1]))
        r0, r1 = run[:n_sh], run[n_sh:]
        k0, k1 = up(r0[:, -1], GRP) // GRP, up(r1[:, -1], GRP) // GRP
        slot0 = jnp.where(m0, r0 - 1, -1)
        slot1 = jnp.where(m1, k0[:, None] * GRP + r1 - 1, -1)
        h0, h1 = k0.reshape(n_half, n_ep), k1.reshape(n_half, n_ep)
        t0, t1 = jnp.sum(h0, axis=1), jnp.sum(h1, axis=1)
        n0, n1 = up(t0, fill) // fill, up(t1, fill) // fill
        base = jnp.arange(n_half, dtype=i32) * (half_t * fill)
        s0 = (base[:, None] + before(h0)).reshape(-1)
        s1 = ((base + n0 * fill)[:, None] + before(h1)).reshape(-1)
        j = jnp.arange(per, dtype=i32)[None, :]
        dst = jnp.where(j < k0[:, None], s0[:, None] + j, jnp.where(j < (k0 + k1)[:, None], s1[:, None] + j - k0[:, None], -1))
        f = jnp.arange(fill, dtype=i32)[None, :]
        gap0 = jnp.where(t0[:, None] + f < (n0 * fill)[:, None], (base + t0)[:, None] + f, -1)
        gap1 = jnp.where(t1[:, None] + f < (n1 * fill)[:, None], (base + n0 * fill + t1)[:, None] + f, -1)
        dst_all = jnp.concatenate([dst.reshape(n_half, -1), gap0, gap1], axis=1).reshape(-1)
        n_fill = 2 * fill // per
        cycle = n_ep + n_fill
        order_h = order.reshape(n_half, n_ep)
        order_all = jnp.concatenate([order_h, jnp.broadcast_to(order_h[:, -1:], (n_half, n_fill))], axis=1).reshape(-1)

        def pad(v, c):
            v = jnp.concatenate([v.reshape(n_half, n_ep, n_tok), jnp.full((n_half, n_fill, n_tok), c, v.dtype)], axis=1)
            return v.reshape(n_half * cycle, 1, n_tok)

        slot0, slot1, p0, p1 = pad(slot0, -1), pad(slot1, -1), pad(p0, 0.0), pad(p1, 0.0)

        na, nb, nc, nd = n0[0], n0[1], n1[0], n1[1]
        total = na + nb + nc + nd
        t = jnp.minimum(jnp.arange(n_half * half_t, dtype=i32), total - 1)
        all_t = jnp.where(t < na, t, jnp.where(t < na + nb, half_t + t - na, jnp.where(t < na + nb + nc, t - nb, half_t + t - na - nc)))
        all_l = (all_t, (t >= na + nb).astype(i32), total[None])
        t = jnp.arange(half_t, dtype=i32)
        tl, to = jnp.minimum(t, na + nc - 1), jnp.minimum(t, nb + nd - 1)
        own_l = (tl, (tl >= na).astype(i32), (na + nc)[None])
        oth_l = (half_t + to, (to >= nb).astype(i32), (nb + nd)[None])

        dst_loc = dst[:n_ep]
        grp = jnp.arange(half_t * fill, dtype=i32)
        inverse = jnp.sum(jnp.where(dst_loc.reshape(-1)[:, None] == grp[None, :], jnp.arange(n_ep * per, dtype=i32)[:, None] + 1, 0), axis=0) - 1

        mine = jnp.concatenate(hot)
        rank = running(mine)
        cnt = rank[:n_exp] + rank[n_exp:]
        kk = up(cnt[:, -1], GRP)
        off = jnp.where(eid % 2 == 1, jnp.concatenate([kk[:1], kk[:-1]]), 0)
        slot = off[:, None] + cnt - 1
        own = [jnp.sum(jnp.where(h, slot, 0), axis=0) for h in hot]
        src = [idx[k] // 2 for k in range(top_k)]
        nat = [src[k] * SLOT + own[k] for k in range(top_k)]
        rel = [src[k] ^ my_ep for k in range(top_k)]
        ret = [
            jnp.where(
                own[k] < BASE,
                rel[k] * BASE + own[k],
                n_ep * BASE + jnp.where(own[k] < BASE + MORE, rel[k] * MORE + own[k] - BASE, (rel[k] ^ 1) * MORE + own[k] - BASE - MORE),
            )[:, None]
            for k in range(top_k)
        ]
        dev = jnp.arange(n_ep, dtype=i32)
        full = kk.reshape(n_ep, 2).sum(axis=1)
        got = jnp.sum(jnp.where((dev ^ my_ep)[:, None] == dev[None, :], full[None, :], 0), axis=1)
        mate = got.reshape(-1, 2)[:, ::-1].reshape(-1)
        valid = jnp.concatenate([jnp.minimum(got, BASE), jnp.where(got > BASE, got - BASE, mate - BASE - MORE)])

        tabs = (order_all, dst_all, slot0, slot1, p0, p1)
        cut = lambda h: [v[h * (v.shape[0] // n_half) : (h + 1) * (v.shape[0] // n_half)] for v in tabs]
        xs, ps = gather_rows(*tabs, x_all, n_rows, n_ep, cycle, True)
        a, a_t, u1, u3 = forward(*all_l, xs, w1, w3)
        g_far, a = lax.optimization_barrier((g_far, a))
        g_far = lax.all_gather(g_far, "ep", axis=0, tiled=True)

        in_half = lambda h: (cut(h)[0] % n_ep, *cut(h)[1:])
        (gs,) = gather_rows(*in_half(0), g_own, n_rows, n_ep, cycle, False)
        d1_t, d3_t, d1, d3, q = hidden_grad(*own_l, gs, ps, a, u1, u3, w_down)

        nat_dst = dst_loc[dev ^ my_ep].reshape(-1)
        q_send = q[: half_t * TILE, 0].reshape(half_t * fill, GRP)[jnp.maximum(nat_dst, 0)].reshape(n_ep, SLOT)
        q_recv = lax.all_to_all(q_send, "ep", 0, 0, tiled=True).reshape(1, n_ep * SLOT)
        spot = jnp.arange(n_ep * SLOT, dtype=i32)[None, :]
        qk = [jnp.sum(jnp.where(spot == nat[k][:, None], q_recv, 0.0), axis=1) for k in range(top_k)]
        mean = probs[0] * qk[0] + probs[1] * qk[1]
        dl = [probs[k] * (qk[k] - mean) for k in range(top_k)]
        d_logits = sum(jnp.where(idx[k][:, None] == eid[None, :], dl[k][:, None], 0.0) for k in range(top_k)).astype(BF)
        part_router = lax.dot_general(d_logits, x_loc, TN_DIMS, preferred_element_type=F32)

        rows = row_grad(*own_l, inverse, d1, d3, w1, w3, n_ep * SLOT, 0, dim).reshape(n_ep, SLOT, dim)
        last = jnp.stack([rows[b ^ 1, BASE + MORE :] for b in range(n_ep)])
        last = lax.ppermute(last, "ep", [(s, s ^ 1) for s in range(n_ep)])
        here = (k0 + k1)[:n_ep] * GRP > BASE
        more = jnp.where(here[:, None, None], rows[:, BASE : BASE + MORE], last)
        parts = [rows[b, :BASE] for b in range(n_ep)] + [more[b] for b in range(n_ep)]
        g_far, part_router, d1_t, d3_t, gs, *parts = lax.optimization_barrier((g_far, part_router, d1_t, d3_t, gs, *parts))
        sent = [p if n % n_ep == 0 else lax.ppermute(p, "ep", [(s, s ^ (n % n_ep)) for s in range(n_ep)]) for n, p in enumerate(parts)]

        (gs,) = gather_rows(*in_half(1), g_far, n_rows, n_ep, cycle, False, into=gs)
        d1_t, d3_t = hidden_grad(*oth_l, gs, ps, a, u1, u3, w_down, into=[d1_t, d3_t])
        o1, o3, o2 = weight_grads(*all_l, xs, gs, ps, a_t, d1_t, d3_t)
        o1, o3, o2, *sent = lax.optimization_barrier((o1, o3, o2, *sent))
        grad_router = lax.psum(part_router, both).T
        grad_x = combine(valid, ret[0], ret[1], d_logits, wr_t, sent)
        return grad_x, jnp.swapaxes(o1, 1, 2), jnp.swapaxes(o3, 1, 2), o2, grad_router

    return jax.shard_map(device_step, mesh=mesh, in_specs=(tok_spec, tok_spec, P(), exp_spec, exp_spec, exp_spec, tok_spec), out_specs=(tok_spec, exp_spec, exp_spec, exp_spec, P()), check_vma=False)
```

```python
import jax
import jax.numpy as jnp
from jax import lax
from jax.experimental import pallas as pl
from jax.experimental.pallas import tpu as pltpu
from jax.sharding import PartitionSpec as P


TILE = 512
GRP = 16
SLOT = 256
BASE = 128
MORE = 64
NT_DIMS = (((1,), (1,)), ((), ()))
TN_DIMS = (((0,), (0,)), ((), ()))
NEAR = 80
VMEM = 63 * 2**20
BF = jnp.bfloat16
F32 = jnp.float32


def params(**kw):
    return pltpu.CompilerParams(vmem_limit_bytes=VMEM, **kw)


def cost(flops, nbytes):
    return pl.CostEstimate(flops=int(flops), bytes_accessed=int(nbytes), transcendentals=0)


def pick_rows(slot0, slot1, n_tok):
    row = lax.broadcasted_iota(jnp.int32, (SLOT, n_tok), 0)
    return row == slot0, row == slot1


def gather_rows(order, dst, slot0, slot1, p0, p1, rows_all, n_rows, real, cycle, with_p, into=None):
    n_steps = order.shape[0]
    n_src = len(rows_all)
    dim = rows_all[0].shape[1]
    per = SLOT // GRP
    chunk = 1024

    def body(order_ref, dst_ref, *rest):
        s0_refs, s1_refs, x_refs, rest = rest[:n_src], rest[n_src : 2 * n_src], rest[2 * n_src : 3 * n_src], rest[3 * n_src :]
        if with_p:
            p0_ref, p1_ref, *rest = rest
        if into is not None:
            rest = rest[1:]
        if with_p:
            o_ref, po_ref, buf, pbuf, sems, psems = rest
        else:
            o_ref, buf, sems = rest
        i = pl.program_id(0)
        now = lax.rem(i, 2)

        def copies(step, half, j):
            d = dst_ref[step * per + j]
            at = pl.multiple_of(jnp.maximum(d, 0) * GRP, GRP)
            out = [pltpu.make_async_copy(buf.at[half, pl.ds(j * GRP, GRP)], o_ref.at[pl.ds(at, GRP)], sems.at[half, j])]
            if with_p:
                out.append(pltpu.make_async_copy(pbuf.at[half, pl.ds(j * GRP, GRP)], po_ref.at[pl.ds(at, GRP)], psems.at[half, j]))
            return d, out

        def each(step, half, wait):
            for j in range(per):
                d, cs = copies(step, half, j)

                @pl.when(d >= 0)
                def _():
                    for c in cs:
                        if wait:
                            c.wait()
                        else:
                            c.start()

        @pl.when(i >= 2)
        def _():
            each(i - 2, now, True)

        picks = [pick_rows(a[0], b[0], a.shape[-1]) for a, b in zip(s0_refs, s1_refs)]
        is_real = lax.rem(i, cycle) < real

        @pl.when(is_real)
        def _():
            pick = [jnp.where(a | b, 1.0, 0.0).astype(BF) for a, b in picks]
            for c in range(dim // chunk):
                cols = pl.ds(c * chunk, chunk)
                buf[now, :, cols] = sum(jnp.dot(p, x[:, cols], preferred_element_type=F32) for p, x in zip(pick, x_refs)).astype(BF)

        @pl.when(jnp.logical_not(is_real))
        def _():
            buf[now] = jnp.zeros((SLOT, dim), BF)

        if with_p:
            p = jnp.where(picks[0][0], p0_ref[0], 0.0) + jnp.where(picks[0][1], p1_ref[0], 0.0)
            pbuf[now] = jnp.broadcast_to(jnp.sum(p, axis=1, keepdims=True), (SLOT, 128))
        each(i, now, False)

        @pl.when(i == n_steps - 1)
        def _():
            each(i - 1, 1 - now, True)
            each(i, now, True)

    vecs = [pl.BlockSpec((1, 1, v.shape[-1]), lambda i, o, d: (i, 0, 0)) for v in slot0]
    wide = [pl.BlockSpec((v.shape[-1], dim), lambda i, o, d: (o[i], 0)) for v in slot0]
    outs = [jax.ShapeDtypeStruct((n_rows, dim), BF)]
    scratch = [pltpu.VMEM((2, SLOT, dim), BF), pltpu.SemaphoreType.DMA((2, per))]
    if with_p:
        outs.append(jax.ShapeDtypeStruct((n_rows, 128), F32))
        scratch = [scratch[0], pltpu.VMEM((2, SLOT, 128), F32), scratch[1], pltpu.SemaphoreType.DMA((2, per))]
    return pl.pallas_call(
        body,
        grid_spec=pltpu.PrefetchScalarGridSpec(
            num_scalar_prefetch=2,
            grid=(n_steps,),
            in_specs=vecs * 2
            + wide
            + (vecs * 2 if with_p else [])
            + ([] if into is None else [pl.BlockSpec(memory_space=pl.ANY)]),
            out_specs=[pl.BlockSpec(memory_space=pl.ANY)] * len(outs),
            scratch_shapes=scratch,
        ),
        out_shape=outs,
        input_output_aliases={} if into is None else {2 + 3 * n_src: 0},
        compiler_params=params(),
        cost_estimate=cost(2 * n_steps * SLOT * 512 * dim, n_steps * (512 + SLOT) * dim * 2),
        name="gather_p" if with_p else "gather_g",
    )(order, dst, *slot0, *slot1, *rows_all, *([p0, p1] if with_p else []), *([] if into is None else [into]))


def forward(tiles, tile_e, n_tiles, xs, w1, w3):
    n_rows, dim = xs.shape
    ff = w1.shape[1]
    nt = tiles.shape[0]

    def body(tl, te, ntr, x_ref, w1_ref, w3_ref, a_ref, at_ref, u1_ref, u3_ref):
        @pl.when(pl.program_id(0) < ntr[0])
        def _():
            z1 = lax.dot_general(x_ref[...], w1_ref[0], NT_DIMS, preferred_element_type=F32)
            z3 = lax.dot_general(x_ref[...], w3_ref[0], NT_DIMS, preferred_element_type=F32)
            sg = jax.nn.sigmoid(z1)
            s = z1 * sg
            a_ref[...] = (s * z3).astype(BF)
            at_ref[...] = a_ref[...].T
            u1_ref[...] = z3 * sg * (1.0 + z1 * (1.0 - sg))
            u3_ref[...] = s

    at = lambda t, tl, te, n: (tl[t], 0)
    wt = pl.BlockSpec((1, ff, dim), lambda t, tl, te, n: (te[t], 0, 0))
    rf = pl.BlockSpec((TILE, ff), at)
    return pl.pallas_call(
        body,
        grid_spec=pltpu.PrefetchScalarGridSpec(
            num_scalar_prefetch=3,
            grid=(nt,),
            in_specs=[pl.BlockSpec((TILE, dim), at), wt, wt],
            out_specs=[rf, pl.BlockSpec((ff, TILE), lambda t, tl, te, n: (0, tl[t])), rf, rf],
        ),
        out_shape=[jax.ShapeDtypeStruct(sh, d) for sh, d in (((n_rows, ff), BF), ((ff, n_rows), BF), ((n_rows, ff), F32), ((n_rows, ff), F32))],
        compiler_params=params(),
        cost_estimate=cost(4 * n_rows * dim * ff, n_rows * dim * 2),
        name="forward",
    )(tiles, tile_e, n_tiles, xs, w1, w3)


def hidden_grad(tiles, tile_e, n_tiles, gs, ps, a, u1, u3, w2, into=None):
    n_rows, dim = gs.shape
    ff = w2.shape[1]
    nt = tiles.shape[0]
    first = into is None

    def body(tl, te, ntr, g_ref, p_ref, a_ref, u1_ref, u3_ref, w_ref, *rest):
        outs = rest if first else rest[2:]

        @pl.when(pl.program_id(0) < ntr[0])
        def _():
            h = lax.dot_general(g_ref[...], w_ref[0], NT_DIMS, preferred_element_type=F32)
            da = p_ref[:, 0:1] * h
            d1 = (da * u1_ref[...]).astype(BF)
            d3 = (da * u3_ref[...]).astype(BF)
            outs[0][...] = d1.T
            outs[1][...] = d3.T
            if first:
                outs[2][...] = d1
                outs[3][...] = d3
                q = jnp.sum(a_ref[...].astype(F32) * h, axis=1, keepdims=True)
                outs[4][...] = jnp.broadcast_to(q, outs[4].shape)

    at = lambda t, tl, te, n: (tl[t], 0)
    rf = pl.BlockSpec((TILE, ff), at)
    lane = pl.BlockSpec((TILE, 128), at)
    turned = pl.BlockSpec((ff, TILE), lambda t, tl, te, n: (0, tl[t]))
    any_spec = pl.BlockSpec(memory_space=pl.ANY)
    return pl.pallas_call(
        body,
        grid_spec=pltpu.PrefetchScalarGridSpec(
            num_scalar_prefetch=3,
            grid=(nt,),
            in_specs=[pl.BlockSpec((TILE, dim), at), lane, rf, rf, rf, pl.BlockSpec((1, ff, dim), lambda t, tl, te, n: (te[t], 0, 0))]
            + ([] if first else [any_spec, any_spec]),
            out_specs=[turned, turned] + ([rf, rf, lane] if first else []),
        ),
        out_shape=[jax.ShapeDtypeStruct((ff, n_rows), BF)] * 2
        + ([jax.ShapeDtypeStruct((n_rows, ff), BF)] * 2 + [jax.ShapeDtypeStruct((n_rows, 128), F32)] if first else []),
        input_output_aliases={} if first else {9: 0, 10: 1},
        compiler_params=params(),
        cost_estimate=cost(2 * nt * TILE * dim * ff, nt * TILE * dim * 2),
        name="hidden_grad",
    )(tiles, tile_e, n_tiles, gs, ps, a, u1, u3, w2, *(into or []))


def row_grad(tiles, tiles_e, n_tiles, inverse, d1, d3, w1, w3, n_out, first, width):
    ff = d1.shape[1]
    nl = tiles.shape[0]
    per = TILE // GRP
    chunk = min(width, 1024)

    def body(tl, te, ntr, inv, d1_ref, d3_ref, w1_ref, w3_ref, o_ref, buf, sems):
        t = pl.program_id(0)
        now = lax.rem(t, 2)

        def each(step, half, wait):
            for j in range(per):
                d = inv[tl[step] * per + j]
                at = pl.multiple_of(jnp.maximum(d, 0) * GRP, GRP)

                @pl.when((step < ntr[0]) & (d >= 0))
                def _():
                    c = pltpu.make_async_copy(buf.at[half, pl.ds(j * GRP, GRP)], o_ref.at[pl.ds(at, GRP)], sems.at[half, j])
                    if wait:
                        c.wait()
                    else:
                        c.start()

        @pl.when(t >= 2)
        def _():
            each(t - 2, now, True)

        @pl.when(t < ntr[0])
        def _():
            for c in range(width // chunk):
                cols = pl.ds(c * chunk, chunk)
                r = jnp.dot(d1_ref[...], w1_ref[0, :, cols], preferred_element_type=F32)
                r += jnp.dot(d3_ref[...], w3_ref[0, :, cols], preferred_element_type=F32)
                buf[now, :, cols] = r.astype(BF)

        each(t, now, False)

        @pl.when(t == nl - 1)
        def _():
            each(t - 1, 1 - now, True)
            each(t, now, True)

    at = pl.BlockSpec((TILE, ff), lambda t, tl, te, n, inv: (tl[t], 0))
    wt = pl.BlockSpec((1, ff, width), lambda t, tl, te, n, inv: (te[t], 0, first // width))
    return pl.pallas_call(
        body,
        grid_spec=pltpu.PrefetchScalarGridSpec(
            num_scalar_prefetch=4,
            grid=(nl,),
            in_specs=[at, at, wt, wt],
            out_specs=pl.BlockSpec(memory_space=pl.ANY),
            scratch_shapes=[pltpu.VMEM((2, TILE, width), BF), pltpu.SemaphoreType.DMA((2, per))],
        ),
        out_shape=jax.ShapeDtypeStruct((n_out, width), BF),
        compiler_params=params(),
        cost_estimate=cost(4 * nl * TILE * width * ff, n_out * width * 2),
        name="row_grad",
    )(tiles, tiles_e, n_tiles, inverse, d1, d3, w1, w3)


def weight_grads(tiles, tile_e, n_tiles, xs, gs, ps, a_t, d1_t, d3_t):
    n_rows, dim = xs.shape
    ff = a_t.shape[0]
    nt = tiles.shape[0]
    cols = 2048
    chunk = 1024

    def body(tl, te, ntr, x_ref, g_ref, p_ref, a_ref, d1_ref, d3_ref, *outs):
        t = pl.program_id(1)
        fresh = (t == 0) | (te[t] != te[jnp.maximum(t - 1, 0)])

        def put(k, at, lhs_t, rhs):
            new = jnp.dot(lhs_t[...], rhs, preferred_element_type=F32)
            outs[k][0, :, at] = jnp.where(fresh, 0.0, outs[k][0, :, at]) + new

        @pl.when(t < ntr[0])
        def _():
            @pl.loop(0, cols // chunk)
            def _(c):
                at = pl.ds(pl.multiple_of(c * chunk, chunk), chunk)
                x = x_ref[:, at]
                put(0, at, d1_ref, x)
                put(1, at, d3_ref, x)
                put(2, at, a_ref, (p_ref[:, 0:1] * g_ref[:, at].astype(F32)).astype(BF))

    wide = pl.BlockSpec((TILE, cols), lambda d, t, tl, te, n: (tl[t], d))
    rf = pl.BlockSpec((ff, TILE), lambda d, t, tl, te, n: (0, tl[t]))
    lane = pl.BlockSpec((TILE, 128), lambda d, t, tl, te, n: (tl[t], 0))
    out = pl.BlockSpec((1, ff, cols), lambda d, t, tl, te, n: (te[t], 0, d))
    return pl.pallas_call(
        body,
        grid_spec=pltpu.PrefetchScalarGridSpec(
            num_scalar_prefetch=3,
            grid=(dim // cols, nt),
            in_specs=[wide, wide, lane, rf, rf, rf],
            out_specs=[out, out, out],
        ),
        out_shape=[jax.ShapeDtypeStruct((2, ff, dim), F32)] * 3,
        compiler_params=params(),
        cost_estimate=cost(6 * nt * TILE * dim * ff, 4 * n_rows * dim + 12 * ff * dim * 2),
        name="weight_grads",
    )(tiles, tile_e, n_tiles, xs, gs, ps, a_t, d1_t, d3_t)


def combine(valid, i0, i1, dl, wr_t, blocks):
    n_tok = i0.shape[0]
    dim = wr_t.shape[1]
    sizes = [b.shape[0] for b in blocks]
    total = sum(sizes)
    cols = 512

    def body(nv, i0_ref, i1_ref, dl_ref, w_ref, *rest):
        refs, o_ref, pick, rows = rest[:-3], rest[-3], rest[-2], rest[-1]

        @pl.when(pl.program_id(0) == 0)
        def _():
            col = lax.broadcasted_iota(jnp.int32, (n_tok, total), 1)
            pick[...] = jnp.where((col == i0_ref[...]) | (col == i1_ref[...]), 1.0, 0.0).astype(BF)

        at = 0
        for b, size in enumerate(sizes):
            row = lax.broadcasted_iota(jnp.int32, (size, cols), 0)
            rows[at : at + size] = jnp.where(row < nv[b], refs[b][...].astype(F32), 0.0).astype(BF)
            at += size
        tot = jnp.dot(pick[...], rows[...], preferred_element_type=F32)
        o_ref[...] = (tot + jnp.dot(dl_ref[...], w_ref[...], preferred_element_type=F32)).astype(BF)

    one = pl.BlockSpec((n_tok, 1), lambda c, nv: (0, 0))
    ins = [one, one, pl.BlockSpec((n_tok, dl.shape[1]), lambda c, nv: (0, 0)), pl.BlockSpec((dl.shape[1], cols), lambda c, nv: (0, c))]
    ins += [pl.BlockSpec((size, cols), lambda c, nv: (0, c)) for size in sizes]
    return pl.pallas_call(
        body,
        grid_spec=pltpu.PrefetchScalarGridSpec(
            num_scalar_prefetch=1,
            grid=(dim // cols,),
            in_specs=ins,
            out_specs=pl.BlockSpec((n_tok, cols), lambda c, nv: (0, c)),
            scratch_shapes=[pltpu.VMEM((n_tok, total), BF), pltpu.VMEM((total, cols), BF)],
        ),
        out_shape=jax.ShapeDtypeStruct((n_tok, dim), BF),
        compiler_params=params(),
        cost_estimate=cost(2 * n_tok * total * dim, total * dim * 2),
        name="combine",
    )(valid, i0, i1, dl, wr_t, *blocks)


def up(v, m):
    return (v + m - 1) // m * m


def before(v):
    i = jnp.arange(v.shape[-1], dtype=jnp.int32)
    return jnp.sum(jnp.where(i[None, None, :] < i[None, :, None], v[:, None, :], 0), axis=2)


def running(mask):
    n = mask.shape[-1]
    i = jnp.arange(n, dtype=jnp.int32)
    tri = (i[:, None] <= i[None, :]).astype(BF)
    return jnp.dot(mask.astype(BF), tri, preferred_element_type=F32).astype(jnp.int32)


def solution(mesh):
    n_dp, n_ep = mesh.shape["dp"], mesh.shape["ep"]
    tok_spec = P(("dp", "ep"), None)
    exp_spec = P("ep", None, None)
    both = ("dp", "ep")

    def device_step(x_loc, route_idx, w_router, w_gate, w_up, w_down, g_loc):
        n_tok, top_k = route_idx.shape
        dim = x_loc.shape[1]
        n_exp = w_router.shape[1]
        my_dp, my_ep = lax.axis_index("dp"), lax.axis_index("ep")
        n_sh = n_dp * n_ep
        per = SLOT // GRP
        fill = TILE // GRP
        n_half = n_dp
        half_t = n_ep * SLOT // TILE + 1
        n_rows = n_half * half_t * TILE
        i32 = jnp.int32

        x_all = lax.all_gather(x_loc, both, axis=0, tiled=True)

        w1 = jnp.swapaxes(w_gate, 1, 2)
        w3 = jnp.swapaxes(w_up, 1, 2)
        wr_t = w_router.T

        logits = lax.dot_general(wr_t, x_loc, NT_DIMS, preferred_element_type=F32)
        idx = route_idx.T
        eid = jnp.arange(n_exp, dtype=i32)
        hot = [idx[k][None, :] == eid[:, None] for k in range(top_k)]
        sel = jnp.stack([jnp.sum(jnp.where(h, logits, 0.0), axis=0) for h in hot])
        probs = jax.nn.softmax(sel, axis=0)
        meta = lax.all_gather(jnp.concatenate([idx.astype(F32), probs]), both, axis=0)

        g_in, meta = lax.optimization_barrier((g_loc, meta))
        g_own = lax.all_gather(g_in, "ep", axis=0, tiled=True)
        g_out, x_all = lax.optimization_barrier((g_loc[NEAR:], x_all))
        g_far = lax.ppermute(g_out, "dp", [(s, (s + 1) % n_dp) for s in range(n_dp)])

        step = jnp.arange(n_sh, dtype=i32)
        order = ((my_dp + step // n_ep) % n_dp) * n_ep + ((step % n_ep) ^ my_ep)
        meta = meta[order]
        i_all, p_all = meta[:, :top_k].astype(i32), meta[:, top_k:]
        e0 = my_ep * 2
        m0 = [i_all[:, k] == e0 for k in range(top_k)]
        m1 = [i_all[:, k] == e0 + 1 for k in range(top_k)]
        m0, m1, p0, p1 = m0[0] | m0[1], m1[0] | m1[1], jnp.where(m0[0], p_all[:, 0], p_all[:, 1]), jnp.where(m1[0], p_all[:, 0], p_all[:, 1])
        run = running(jnp.concatenate([m0, m1]))
        r0, r1 = run[:n_sh], run[n_sh:]
        k0, k1 = up(r0[:, -1], GRP) // GRP, up(r1[:, -1], GRP) // GRP
        slot0 = jnp.where(m0, r0 - 1, -1)
        slot1 = jnp.where(m1, k0[:, None] * GRP + r1 - 1, -1)
        h0, h1 = k0.reshape(n_half, n_ep), k1.reshape(n_half, n_ep)
        t0, t1 = jnp.sum(h0, axis=1), jnp.sum(h1, axis=1)
        n0, n1 = up(t0, fill) // fill, up(t1, fill) // fill
        base = jnp.arange(n_half, dtype=i32) * (half_t * fill)
        s0 = (base[:, None] + before(h0)).reshape(-1)
        s1 = ((base + n0 * fill)[:, None] + before(h1)).reshape(-1)
        j = jnp.arange(per, dtype=i32)[None, :]
        dst = jnp.where(j < k0[:, None], s0[:, None] + j, jnp.where(j < (k0 + k1)[:, None], s1[:, None] + j - k0[:, None], -1))
        f = jnp.arange(fill, dtype=i32)[None, :]
        gap0 = jnp.where(t0[:, None] + f < (n0 * fill)[:, None], (base + t0)[:, None] + f, -1)
        gap1 = jnp.where(t1[:, None] + f < (n1 * fill)[:, None], (base + n0 * fill + t1)[:, None] + f, -1)
        dst_all = jnp.concatenate([dst.reshape(n_half, -1), gap0, gap1], axis=1).reshape(-1)
        n_fill = 2 * fill // per
        cycle = n_ep + n_fill
        order_h = order.reshape(n_half, n_ep)
        order_all = jnp.concatenate([order_h, jnp.broadcast_to(order_h[:, -1:], (n_half, n_fill))], axis=1).reshape(-1)

        def pad(v, c):
            v = jnp.concatenate([v.reshape(n_half, n_ep, n_tok), jnp.full((n_half, n_fill, n_tok), c, v.dtype)], axis=1)
            return v.reshape(n_half * cycle, 1, n_tok)

        slot0, slot1, p0, p1 = pad(slot0, -1), pad(slot1, -1), pad(p0, 0.0), pad(p1, 0.0)

        na, nb, nc, nd = n0[0], n0[1], n1[0], n1[1]
        total = na + nb + nc + nd
        t = jnp.minimum(jnp.arange(n_half * half_t, dtype=i32), total - 1)
        all_t = jnp.where(t < na, t, jnp.where(t < na + nb, half_t + t - na, jnp.where(t < na + nb + nc, t - nb, half_t + t - na - nc)))
        all_l = (all_t, (t >= na + nb).astype(i32), total[None])
        t = jnp.arange(half_t, dtype=i32)
        tl, to = jnp.minimum(t, na + nc - 1), jnp.minimum(t, nb + nd - 1)
        own_l = (tl, (tl >= na).astype(i32), (na + nc)[None])
        oth_l = (half_t + to, (to >= nb).astype(i32), (nb + nd)[None])

        dst_loc = dst[:n_ep]
        grp = jnp.arange(half_t * fill, dtype=i32)
        inverse = jnp.sum(jnp.where(dst_loc.reshape(-1)[:, None] == grp[None, :], jnp.arange(n_ep * per, dtype=i32)[:, None] + 1, 0), axis=0) - 1

        mine = jnp.concatenate(hot)
        rank = running(mine)
        cnt = rank[:n_exp] + rank[n_exp:]
        kk = up(cnt[:, -1], GRP)
        off = jnp.where(eid % 2 == 1, jnp.concatenate([kk[:1], kk[:-1]]), 0)
        slot = off[:, None] + cnt - 1
        own = [jnp.sum(jnp.where(h, slot, 0), axis=0) for h in hot]
        src = [idx[k] // 2 for k in range(top_k)]
        nat = [src[k] * SLOT + own[k] for k in range(top_k)]
        rel = [src[k] ^ my_ep for k in range(top_k)]
        ret = [
            jnp.where(
                own[k] < BASE,
                rel[k] * BASE + own[k],
                n_ep * BASE + jnp.where(own[k] < BASE + MORE, rel[k] * MORE + own[k] - BASE, (rel[k] ^ 1) * MORE + own[k] - BASE - MORE),
            )[:, None]
            for k in range(top_k)
        ]
        dev = jnp.arange(n_ep, dtype=i32)
        full = kk.reshape(n_ep, 2).sum(axis=1)
        got = jnp.sum(jnp.where((dev ^ my_ep)[:, None] == dev[None, :], full[None, :], 0), axis=1)
        mate = got.reshape(-1, 2)[:, ::-1].reshape(-1)
        valid = jnp.concatenate([jnp.minimum(got, BASE), jnp.where(got > BASE, got - BASE, mate - BASE - MORE)])

        tabs = (order_all, dst_all, slot0, slot1, p0, p1)
        cut = lambda h: [v[h * (v.shape[0] // n_half) : (h + 1) * (v.shape[0] // n_half)] for v in tabs]
        xs, ps = gather_rows(order_all, dst_all, [slot0], [slot1], p0, p1, [x_all], n_rows, n_ep, cycle, True)
        a, a_t, u1, u3 = forward(*all_l, xs, w1, w3)
        g_far, a = lax.optimization_barrier((g_far, a))
        g_far = lax.all_gather(g_far, "ep", axis=0, tiled=True)

        near = g_own.reshape(n_ep, n_tok, dim)[:, :NEAR].reshape(n_ep * NEAR, dim)
        near, g_own = lax.optimization_barrier((near, g_own))
        near = lax.ppermute(near, "dp", [(s, (s + 1) % n_dp) for s in range(n_dp)])

        def pick_g(h, cuts, sources, into=None):
            order_c, dst_c, slot0_c, slot1_c, _, _ = cut(h)
            split = lambda v: [v[:, :, a:b] for a, b in cuts]
            return gather_rows(order_c % n_ep, dst_c, split(slot0_c), split(slot1_c), None, None, sources, n_rows, n_ep, cycle, False, into)

        (gs,) = pick_g(0, [(0, n_tok)], [g_own])
        d1_t, d3_t, d1, d3, q = hidden_grad(*own_l, gs, ps, a, u1, u3, w_down)

        nat_dst = dst_loc[dev ^ my_ep].reshape(-1)
        q_send = q[: half_t * TILE, 0].reshape(half_t * fill, GRP)[jnp.maximum(nat_dst, 0)].reshape(n_ep, SLOT)
        q_recv = lax.all_to_all(q_send, "ep", 0, 0, tiled=True).reshape(1, n_ep * SLOT)
        spot = jnp.arange(n_ep * SLOT, dtype=i32)[None, :]
        qk = [jnp.sum(jnp.where(spot == nat[k][:, None], q_recv, 0.0), axis=1) for k in range(top_k)]
        mean = probs[0] * qk[0] + probs[1] * qk[1]
        dl = [probs[k] * (qk[k] - mean) for k in range(top_k)]
        d_logits = sum(jnp.where(idx[k][:, None] == eid[None, :], dl[k][:, None], 0.0) for k in range(top_k)).astype(BF)
        part_router = lax.dot_general(d_logits, x_loc, TN_DIMS, preferred_element_type=F32)

        rows = row_grad(*own_l, inverse, d1, d3, w1, w3, n_ep * SLOT, 0, dim).reshape(n_ep, SLOT, dim)
        last = jnp.stack([rows[b ^ 1, BASE + MORE :] for b in range(n_ep)])
        last = lax.ppermute(last, "ep", [(s, s ^ 1) for s in range(n_ep)])
        here = (k0 + k1)[:n_ep] * GRP > BASE
        more = jnp.where(here[:, None, None], rows[:, BASE : BASE + MORE], last)
        parts = [rows[b, :BASE] for b in range(n_ep)] + [more[b] for b in range(n_ep)]
        near, g_far, part_router, d1_t, d3_t, gs, *parts = lax.optimization_barrier((near, g_far, part_router, d1_t, d3_t, gs, *parts))
        sent = [p if n % n_ep == 0 else lax.ppermute(p, "ep", [(s, s ^ (n % n_ep)) for s in range(n_ep)]) for n, p in enumerate(parts)]

        (gs,) = pick_g(1, [(0, NEAR), (NEAR, n_tok)], [near, g_far], into=gs)
        d1_t, d3_t = hidden_grad(*oth_l, gs, ps, a, u1, u3, w_down, into=[d1_t, d3_t])
        o1, o3, o2 = weight_grads(*all_l, xs, gs, ps, a_t, d1_t, d3_t)
        o1, o3, o2, *sent = lax.optimization_barrier((o1, o3, o2, *sent))
        grad_router = lax.psum(part_router, both).T
        grad_x = combine(valid, ret[0], ret[1], d_logits, wr_t, sent)
        return grad_x, jnp.swapaxes(o1, 1, 2), jnp.swapaxes(o3, 1, 2), o2, grad_router

    return jax.shard_map(device_step, mesh=mesh, in_specs=(tok_spec, tok_spec, P(), exp_spec, exp_spec, exp_spec, tok_spec), out_specs=(tok_spec, exp_spec, exp_spec, exp_spec, P()), check_vma=False)
```
